32 devices in a mesh: iface: 8 (over z, y), dom: 4 (over x, core).
Axes of the slice: x: 2, y: 2, z: 4, core: 2. Of those that a mesh axis runs over, the one named last changes fastest.
Arguments:
- interface: float32 [131072], P(('iface', 'dom')), may hold values from -6 to 6
- previous_residual: float32 [131072], P(('iface', 'dom')), may hold values from -6 to 6
- previous_estimate: float32 [131072], P(('iface', 'dom')), may hold values from -6 to 6
- forcing: float32 [131072], P(('iface', 'dom')), may hold values from -60 to 60
- stiffness: float32 [131072], P(('iface', 'dom')), may hold values from 0.2 to 0.6
- history_residual: float32 [100, 131072], P(None, ('iface', 'dom')), may hold values from -40 to 40
- history_estimate: float32 [100, 131072], P(None, ('iface', 'dom')), may hold values from -6 to 6
Outputs:
- interface_next: float32 [131072], P(('iface', 'dom'))
- residual_last: float32 [131072], P(('iface', 'dom'))
The draws below stay inside these ranges and needn't reach their ends.
All inputs are finite; a program needn't handle non-finite values.
Results may differ from the reference program's by a relative error of at most 0.0003.
Values sent between devices are 32-bit elements; how exact they have to be, the bound alone decides.
A program may use at most 64 MiB of HBM per device.

```python
import math
import jax
import jax.numpy as jnp
from jax import lax

HIST = 100
ITERS = 3
NI = 131072


def shared_history(key):
    high = lax.Precision.HIGHEST
    base = jax.random.normal(jax.random.fold_in(key, 7), (HIST + 1, NI), jnp.float32)
    factors = jax.random.uniform(jax.random.fold_in(key, 11), (HIST, 1), jnp.float32, 0.4, 0.8)
    banded = base[1:] + factors * base[:-1]
    mixing = jnp.eye(HIST, dtype=jnp.float32) + 0.2 * jax.random.normal(jax.random.fold_in(key, 12), (HIST, HIST), jnp.float32) / math.sqrt(HIST)
    mixed = jnp.dot(mixing, banded, precision=high)
    return jnp.clip(mixed, -40.0, 40.0)


def draw_history_residual(key, part):
    return shared_history(key)


def draw_forcing(key, part):
    mixed = shared_history(key)
    weights = jax.random.normal(jax.random.fold_in(key, 9), (HIST,), jnp.float32) / math.sqrt(HIST)
    noise = jax.random.normal(jax.random.fold_in(key, 10), (NI,), jnp.float32)
    total = 0.8 * jnp.dot(weights, mixed, precision=lax.Precision.HIGHEST) + 0.5 * noise
    return jnp.clip(total, -60.0, 60.0)


def shard_levels(key, shape, pieces, least, high):
    level = 1.0
    for axis_at, shards_of in pieces:
        steps = jax.random.uniform(jax.random.fold_in(jax.random.fold_in(key, 6), axis_at), (shards_of,), jnp.float32, least / len(pieces), high / len(pieces))
        level = level * jnp.repeat(jnp.exp(steps), shape[axis_at] // shards_of).reshape((-1,) + (1,) * (len(shape) - 1 - axis_at))
    return level


def normal_values(rng, shape, deviation, most, shards=(), kind=jnp.bfloat16):
    loudness = shard_levels(rng, shape, shards, -0.22, 0.18) if shards else 1.0
    drawn = jax.random.normal(rng, shape, jnp.float32) * deviation * loudness
    return jnp.minimum(jnp.maximum(drawn, -most), most).astype(kind)


def setup_inputs(seed: int = 0) -> dict:
    streams_of = jax.random.split(jax.random.key(seed), 8)
    interface = normal_values(streams_of[0], (NI,), 1.0, 6.0, ((0, 32),), jnp.float32)
    previous_residual = normal_values(streams_of[1], (NI,), 1.0, 6.0, ((0, 32),), jnp.float32)
    previous_estimate = normal_values(streams_of[2], (NI,), 1.0, 6.0, ((0, 32),), jnp.float32)
    forcing = draw_forcing(jax.random.fold_in(streams_of[7], 71), 0)
    stiffness = jnp.clip(0.2 + 0.400000021 * jax.random.uniform(streams_of[4], (NI,), jnp.float32) ** shard_levels(streams_of[4], (NI,), ((0, 32),), -0.2, 0.2), 0.2, 0.6)
    history_residual = draw_history_residual(jax.random.fold_in(streams_of[7], 71), 0)
    history_estimate = normal_values(streams_of[6], (HIST, NI), 1.0, 6.0, ((1, 32),), jnp.float32)
    return dict(interface=interface, previous_residual=previous_residual, previous_estimate=previous_estimate, forcing=forcing, stiffness=stiffness, history_residual=history_residual, history_estimate=history_estimate)


coupling = 0.25

def solver_map(current, forcing, stiffness):
    padded = jnp.pad(current, 1)
    return forcing + stiffness * jnp.tanh(current) + coupling * (padded[:-2] + padded[2:])

def reference(interface, previous_residual, previous_estimate, forcing, stiffness, history_residual, history_estimate):
    high = lax.Precision.HIGHEST
    current = interface
    hist_v = history_residual
    hist_w = history_estimate
    old_residual = previous_residual
    old_estimate = previous_estimate
    residual = previous_residual
    for iteration in range(ITERS):
        estimate = solver_map(current, forcing, stiffness)
        residual = estimate - current
        hist_v = jnp.concatenate([hist_v, (residual - old_residual)[None, :]], axis=0)
        hist_w = jnp.concatenate([hist_w, (estimate - old_estimate)[None, :]], axis=0)
        gram_matrix = jnp.dot(hist_v, hist_v.T, precision=high)
        projection = jnp.dot(hist_v, residual, precision=high)
        factor = jnp.linalg.cholesky(gram_matrix)
        coeffs = -jax.scipy.linalg.cho_solve((factor, True), projection)
        current = estimate + jnp.dot(coeffs, hist_w, precision=high)
        old_residual = residual
        old_estimate = estimate
    return (current, residual)
```

```python
import functools
import jax
import jax.numpy as jnp
from jax import lax
from jax.experimental import pallas as pl
from jax.experimental.pallas import tpu as pltpu
from jax.sharding import PartitionSpec as P

ITERS = 3
coupling = 0.25
LANES = 128
AXES = ("iface", "dom")
F32 = jnp.float32
BF16 = jnp.bfloat16


def invert(matrix, rows):
    lane8 = lax.broadcasted_iota(jnp.int32, (8, LANES), 1)
    sub8 = lax.broadcasted_iota(jnp.int32, (8, LANES), 0)
    blocks = [matrix[8 * at : 8 * at + 8, :] for at in range(rows // 8)]
    for step in range(rows // 8):
        first = 8 * step
        inside = (lane8 >= first) & (lane8 < first + 8)
        unit = (lane8 - first == sub8).astype(F32)
        pivots = blocks[step]
        columns = [jnp.broadcast_to(pivots[:, first + at : first + at + 1], (8, LANES)) for at in range(8)]
        panel = jnp.where(inside, unit, pivots)
        for at in range(8):
            inverse = 1.0 / columns[at][at : at + 1, :]
            own = sub8 == at
            factor = columns[at]
            row = panel[at : at + 1, :] * inverse
            panel = jnp.where(own, row, panel - factor * row)
            for later in range(at + 1, 8):
                row = columns[later][at : at + 1, :] * inverse
                columns[later] = jnp.where(own, row, columns[later] - factor * row)
        for other in range(rows // 8):
            if other != step:
                block = blocks[other]
                total = jnp.where(inside, 0.0, block)
                for at in range(8):
                    column = jnp.broadcast_to(block[:, first + at : first + at + 1], (8, LANES))
                    total = total - column * panel[at : at + 1, :]
                blocks[other] = total
        blocks[step] = panel
    return jnp.concatenate(blocks, axis=0)


def kernel(
    sizes,
    interface,
    previous_residual,
    previous_estimate,
    forcing,
    stiffness,
    history_residual,
    history_estimate,
    next_ref,
    last_ref,
    cur,
    est,
    force,
    stiff,
    old_res,
    hist_v,
    hist_w,
    halo_w,
    new_v,
    new_w,
    edge_out,
    edge_in,
    dots_in,
    square,
    part_out,
    part_in,
    gathered,
    first_in,
    row_in,
    piece_sem,
    load_sem,
    edge_sem,
    wide_sem,
    part_sem,
    gather_sem,
    row_sem,
    go_sem,
):
    n_iface, n_dom, hist, base, rows, width, owners, share, depth = sizes
    count = n_iface * n_dom
    groups = width // LANES
    tall = groups + 8
    at_iface, at_dom = lax.axis_index("iface"), lax.axis_index("dom")
    me = at_iface * n_dom + at_dom
    last = count - 1
    n_own = len(owners)
    ifaces = [lax.rem(at_iface + step, n_iface) for step in range(n_iface)]
    doms = [lax.rem(at_dom + step, n_dom) for step in range(n_dom)]
    everyone = [(a, b) for a in ifaces for b in doms][1:]
    mine = [(at_iface == a) & (at_dom == b) for a, b in owners]
    owner = functools.reduce(jnp.logical_or, mine)
    slot = sum(jnp.where(yes, at, 0) for at, yes in enumerate(mine))

    def place(index):
        return (index // n_dom, lax.rem(index, n_dom))

    right = place(lax.rem(me + 1, count))
    left = place(lax.rem(me + last, count))

    def piece(at):
        span = pl.ds(at * depth, depth)
        return pltpu.make_async_copy(history_residual.at[:, span], hist_v.at[:, span], piece_sem.at[at])

    for at in range(width // depth):
        piece(at).start()
    inside = pl.ds(0, groups)
    small = []
    for at, (source, target) in enumerate(
        [
            (interface, cur.at[inside]),
            (previous_estimate, est.at[inside]),
            (forcing, force.at[inside]),
            (stiffness, stiff.at[inside]),
            (previous_residual, old_res),
        ]
    ):
        copy = pltpu.make_async_copy(source, target, load_sem.at[1 + at])
        copy.start()
        small.append(copy)
    load_w = pltpu.make_async_copy(history_estimate, hist_w, load_sem.at[0])

    barrier = pltpu.get_barrier_semaphore()

    def greet(device):
        pl.semaphore_signal(barrier, inc=1, device_id=device, device_id_type=pl.DeviceIdType.MESH)

    greet(right)
    greet(left)

    @pl.when(owner)
    def _():
        for device in everyone:
            greet(device)

    @pl.when(jnp.logical_not(owner))
    def _():
        for device in owners:
            greet(device)

    main = side = None
    dims = (((1,), (1,)), ((), ()))
    for at in range(width // depth):
        piece(at).wait()
        block = hist_v[:, at * depth : (at + 1) * depth]
        one = block.astype(BF16)
        rest = block - one.astype(F32)
        two = rest.astype(BF16)
        three = (rest - two.astype(F32)).astype(BF16)
        for a, b, which in [(one, one, 0), (two, two, 0), (two, one, 1), (three, one, 1)]:
            term = lax.dot_general(a, b, dims, preferred_element_type=F32)
            if which == 0:
                main = term if main is None else main + term
            else:
                side = term if side is None else side + term
    load_w.start()
    square[...] = jnp.zeros(square.shape, F32)
    square[0:hist, 0:hist] = side
    mirrored = square[...].T
    square[0:hist, 0:hist] = main + side
    square[...] = square[...] + mirrored
    lane8 = lax.broadcasted_iota(jnp.int32, (8, LANES), 1)
    sub8 = lax.broadcasted_iota(jnp.int32, (8, LANES), 0)
    blocks = (base // 8 + 1) // 2 * 2
    pairs = blocks // 2

    def natural(block):
        return (lane8 >= 8 * block) & (lane8 < 8 * blocks)

    for pair in range(n_own * share):
        where = (pair // share, pl.ds(8 * (pair % share), 8), slice(None))
        if pair < pairs:
            other = blocks - 1 - pair
            moved = pltpu.roll(square[8 * other : 8 * other + 8, :], 8 * pair + 8, 1)
            part_out[where] = jnp.where(natural(pair), square[8 * pair : 8 * pair + 8, :], moved)
        else:
            part_out[where] = jnp.zeros((8, LANES), F32)
    for copy in small:
        copy.wait()
    for at, ref in enumerate([cur, est, force, stiff]):
        edge_out[0, at : at + 1] = ref[groups - 1 : groups]
        edge_out[1, at : at + 1] = ref[0:1]
    pl.semaphore_wait(barrier, jnp.where(owner, last, n_own) + 2)

    def remote(source, target, send_sem, recv_sem, device):
        return pltpu.make_async_remote_copy(
            src_ref=source,
            dst_ref=target,
            send_sem=send_sem,
            recv_sem=recv_sem,
            device_id=device,
            device_id_type=pl.DeviceIdType.MESH,
        )

    def send(source, target, sems, device):
        remote(source, target, sems.at[0], sems.at[1], device).start()

    def drain(target, many, sem):
        most = target.at[pl.ds(0, many)]
        pltpu.make_async_copy(most, most, sem).wait()

    def edges(sources, target, sems):
        return [
            remote(source, target.at[side], sems.at[0, side], sems.at[1, side], device)
            for side, (source, device) in enumerate(zip(sources, [right, left]))
        ]

    def edges_start(copies):
        for side, some in enumerate([me < last, me > 0]):

            @pl.when(some)
            def _():
                copies[side].start()

    def edges_wait(copies):
        for side, (sent, received) in enumerate([(me < last, me > 0), (me > 0, me < last)]):

            @pl.when(sent)
            def _():
                copies[side].wait_send()

            @pl.when(received)
            def _():
                copies[side].wait_recv()

    for at, yes in enumerate(mine):

        @pl.when(yes)
        def _():
            part_in[me] = part_out[at]

        @pl.when(jnp.logical_not(yes))
        def _():
            send(part_out.at[at], part_in.at[me], part_sem, owners[at])

    @pl.when(mine[0])
    def _():
        for device in everyone:
            pl.semaphore_signal(go_sem, inc=1, device_id=device, device_id_type=pl.DeviceIdType.MESH)

    halos = edges([edge_out.at[0], edge_out.at[1]], edge_in, edge_sem)
    edges_start(halos)
    tail = pl.ds(width - LANES, LANES)
    head = pl.ds(0, LANES)
    wide = edges([hist_w.at[:, tail], hist_w.at[:, head]], halo_w, wide_sem)

    half = LANES // 2
    from_right = lane8 < half
    valid = (from_right & (me < last)) | ((lane8 >= half) & (me > 0))
    row_at = lax.broadcasted_iota(jnp.int32, (rows, LANES), 0)
    lane_at = lax.broadcasted_iota(jnp.int32, (rows, LANES), 1)
    eye = (row_at == lane_at).astype(F32)

    def column_of(row):
        return jnp.broadcast_to(jnp.sum(eye * row, axis=1, keepdims=True), (rows, LANES))

    def over_rows(value):
        return jnp.sum(value, axis=0, keepdims=True)

    def as_block(row):
        return jnp.broadcast_to(row, (8, LANES))

    def project(refs):
        def add(at, totals):
            first = pl.multiple_of(8 * at, 8)
            chunks = [ref[pl.ds(first, 8), :] for ref in refs]
            totals = list(totals)
            for inner in range(8):
                column = pl.ds(pl.multiple_of((8 * at + inner) * LANES, LANES), LANES)
                block = hist_v[:, column]
                for which, chunk in enumerate(chunks):
                    totals[which] = totals[which] + block * chunk[inner : inner + 1, :]
            return tuple(totals)

        zero = jnp.zeros((hist, LANES), F32)
        return lax.fori_loop(0, groups // 8, add, (zero,) * len(refs))

    def lane_sums(value):
        return over_rows(jnp.concatenate([value, jnp.zeros((LANES - value.shape[0], LANES), F32)], axis=0).T)

    def begin(iteration):
        if iteration == 0:
            totals_before = project([old_res])[0]
        current = cur[...]
        sides = []
        for shift, edge_lane in [(1, 0), (-1, LANES - 1)]:
            rolled = pltpu.roll(current, shift % LANES, 1)
            moved = pltpu.roll(rolled, shift % tall, 0)
            lane = lax.broadcasted_iota(jnp.int32, (tall, LANES), 1)
            sides.append(jnp.where(lane == edge_lane, moved, rolled))
        estimate = force[...] + stiff[...] * jnp.tanh(current) + coupling * (sides[0] + sides[1])
        new_w[iteration] = estimate - est[...]
        est[...] = estimate
        residual = (estimate - current)[0:groups]
        fresh = residual - old_res[...]
        new_v[iteration] = fresh
        old_res[...] = residual
        extra = jnp.zeros((8, LANES), F32)
        for other in range(iteration + 1):
            row = fresh if other == iteration else new_v[other]
            for first, value in [(0, residual), (4, fresh)]:
                extra = jnp.where(sub8 == first + other, over_rows(row * value), extra)
        total = project([old_res])[0]
        sums = lane_sums(jnp.concatenate([total, jnp.zeros((base - hist, LANES), F32), extra], axis=0))
        dots_in[iteration, 0:1] = sums
        target = row_in.at[iteration - 1]
        source = dots_in.at[iteration, pl.ds(0, 1)]
        if iteration == 0:
            dots_in[0, 1:2] = lane_sums(totals_before)
            target, source = first_in, dots_in.at[0]

            @pl.when(jnp.logical_not(mine[0]))
            def _():
                pl.semaphore_wait(go_sem, 1)

            first_in[me] = dots_in[0]
        else:
            row_in[iteration - 1, me] = sums
        for device in everyone:
            send(source, target.at[me], row_sem.at[iteration], device)

    def sums_of(iteration):
        target = first_in if iteration == 0 else row_in.at[iteration - 1]
        drain(target, last, row_sem.at[iteration, 1])
        return jnp.sum(target[...], axis=0)

    edges_wait(halos)
    for at, ref in enumerate([cur, est, force, stiff]):
        both = jnp.where(from_right, edge_in[1, at : at + 1], edge_in[0, at : at + 1])
        ref[groups:tall] = jnp.where(valid, both, 0.0)
    begin(0)
    load_w.wait()
    edges_start(wide)

    @pl.when(owner)
    def _():
        drain(part_in, last, part_sem.at[1])
        gathered[slot] = jnp.sum(part_in[...], axis=0)
        for device in everyone:
            send(gathered.at[slot], gathered.at[slot], gather_sem, device)
        drain(gathered, n_own - 1, gather_sem.at[1])

    @pl.when(jnp.logical_not(owner))
    def _():
        drain(gathered, n_own, gather_sem.at[1])

    for pair in range(pairs):
        other = blocks - 1 - pair
        packed = gathered[pair // share, pl.ds(8 * (pair % share), 8), :]
        square[8 * pair : 8 * pair + 8, :] = jnp.where(natural(pair), packed, 0.0)
        moved = pltpu.roll(packed, LANES - 8 * pair - 8, 1)
        square[8 * other : 8 * other + 8, :] = jnp.where(natural(other), moved, 0.0)
    upper = square[...]
    lane_block = lax.broadcasted_iota(jnp.int32, (LANES, LANES), 1) // 8
    row_block = lax.broadcasted_iota(jnp.int32, (LANES, LANES), 0) // 8
    square[...] = jnp.where(lane_block >= row_block, upper, upper.T)
    kept = (row_at < hist) & (lane_at < hist)
    square[0:rows, :] = jnp.where(kept, square[0:rows, :], eye)
    square[0:base, :] = invert(square, base)
    square[0:rows, :] = jnp.where(kept, square[0:rows, :], 0.0)
    edges_wait(wide)
    halo_w[0] = jnp.where(
        lax.broadcasted_iota(jnp.int32, (hist, LANES), 1) < half, halo_w[1], halo_w[0]
    )

    def fold(parts):
        for step in (1, 2, 4):
            low = lax.rem(sub8, 2 * step) < step
            parts = [
                jnp.where(low, a, b) + pltpu.roll(jnp.where(low, b, a), step, 0)
                for a, b in zip(parts[0::2], parts[1::2])
            ]
        return parts[0]

    def solve(row):
        return jnp.broadcast_to(jnp.sum(square[0:base, :] * row, axis=1, keepdims=True), (base, LANES))

    solved, columns, lower, scale = [], [], [], []
    for iteration in range(ITERS):
        both = sums_of(iteration)
        proj = both[0:1, :]
        proj_sol = solve(proj)
        proj_col = column_of(proj)
        extra = proj_col[base:rows]
        proj_col = proj_col[0:base]
        if iteration == 0:
            before_sol, before_col = solve(both[1:2, :]), column_of(both[1:2, :])[0:base]
        solved.append(proj_sol - before_sol)
        columns.append(proj_col - before_col)
        before_sol, before_col = proj_sol, proj_col
        size = iteration + 1
        ahead = []
        for b in range(size):
            value = extra[4 + b : 5 + b, :] - over_rows(columns[b] * solved[iteration])
            for c in range(b if b < iteration else 0):
                value = value - ahead[c] * lower[b][c]
            ahead.append(value)
        lower.append([ahead[b] * scale[b] for b in range(iteration)])
        pivot = ahead[iteration]
        for b in range(iteration):
            pivot = pivot - ahead[b] * lower[iteration][b]
        scale.append(1.0 / pivot)
        answer = []
        for a in range(size):
            value = extra[a : a + 1, :] - over_rows(solved[a] * proj_col)
            for b in range(a):
                value = value - lower[a][b] * answer[b]
            answer.append(value)
        answer = [value * scale[a] for a, value in enumerate(answer)]
        for a in reversed(range(size)):
            for b in range(a + 1, size):
                answer[a] = answer[a] - lower[b][a] * answer[b]
        weights = proj_sol
        for a in range(size):
            weights = weights - solved[a] * answer[a]

        def weighted(ref, column):
            total = None
            for first in range(0, hist, 8):
                some = min(8, hist - first)
                term = ref[first : first + some, column] * weights[first : first + some, :]
                if some < 8:
                    term = jnp.concatenate([term, jnp.zeros((8 - some, LANES), F32)], axis=0)
                total = term if total is None else total + term
            return total

        def finished(where, total):
            for a in range(size):
                total = total + new_w[a, where, :] * answer[a]
            return est[where, :] - total

        def combine(at, carry):
            parts = [
                weighted(hist_w, pl.ds(pl.multiple_of((8 * at + inner) * LANES, LANES), LANES)) for inner in range(8)
            ]
            where = pl.ds(pl.multiple_of(8 * at, 8), 8)
            cur[where, :] = finished(where, fold(parts))
            return carry

        lax.fori_loop(0, groups // 8, combine, 0)
        if iteration + 1 < ITERS:
            edge = as_block(over_rows(weighted(halo_w.at[0], slice(None))))
            cur[groups:tall] = jnp.where(valid, finished(pl.ds(groups, 8), edge), 0.0)
            begin(iteration + 1)
    next_ref[...] = cur[0:groups]
    last_ref[...] = old_res[...]

    @pl.when(owner)
    def _():
        drain(gathered, n_own - 1, part_sem.at[0])
        drain(part_in, last, gather_sem.at[0])

    @pl.when(jnp.logical_not(owner))
    def _():
        drain(gathered, n_own, part_sem.at[0])

    drain(first_in, last, row_sem.at[0, 0])
    for iteration in range(1, ITERS):
        drain(row_in.at[iteration - 1], last, row_sem.at[iteration, 0])


def shards(n_iface, n_dom, *args):
    width = args[0].shape[0]
    hist = args[5].shape[0]
    base = -(-hist // 8) * 8
    rows = base + 8
    count = n_iface * n_dom
    pairs = (base // 8 + 1) // 2
    middle = range(n_iface // 4, n_iface // 4 + max(1, n_iface // 2))
    owners = [(a, b) for a in middle for b in range(n_dom) if b % 2 == (n_dom > 1)][:pairs]
    share = -(-pairs // len(owners))
    depth = next(d for d in (2048, 1024) if width % d == 0)
    groups = width // LANES
    tall = groups + 8
    assert hist <= 112 and ITERS <= 4
    vectors = [a.reshape(groups, LANES) for a in args[:5]]
    any_spec = pl.BlockSpec(memory_space=pl.ANY)
    vmem_spec = pl.BlockSpec(memory_space=pltpu.VMEM)
    outs = pl.pallas_call(
        functools.partial(kernel, (n_iface, n_dom, hist, base, rows, width, owners, share, depth)),
        out_shape=[pltpu.VMEM((groups, LANES), F32)] * 2,
        in_specs=[any_spec] * 7,
        out_specs=[vmem_spec] * 2,
        scratch_shapes=[
            pltpu.VMEM((tall, LANES), F32),
            pltpu.VMEM((tall, LANES), F32),
            pltpu.VMEM((tall, LANES), F32),
            pltpu.VMEM((tall, LANES), F32),
            pltpu.VMEM((groups, LANES), F32),
            pltpu.VMEM((hist, width), F32),
            pltpu.VMEM((hist, width), F32),
            pltpu.VMEM((2, hist, LANES), F32),
            pltpu.VMEM((ITERS, groups, LANES), F32),
            pltpu.VMEM((ITERS, tall, LANES), F32),
            pltpu.VMEM((2, 8, LANES), F32),
            pltpu.VMEM((2, 8, LANES), F32),
            pltpu.VMEM((ITERS, 2, LANES), F32),
            pltpu.VMEM((LANES, LANES), F32),
            pltpu.VMEM((len(owners), 8 * share, LANES), F32),
            pltpu.VMEM((count, 8 * share, LANES), F32),
            pltpu.VMEM((len(owners), 8 * share, LANES), F32),
            pltpu.VMEM((count, 2, LANES), F32),
            pltpu.VMEM((ITERS - 1, count, 1, LANES), F32),
            pltpu.SemaphoreType.DMA((width // depth,)),
            pltpu.SemaphoreType.DMA((6,)),
            pltpu.SemaphoreType.DMA((2, 2)),
            pltpu.SemaphoreType.DMA((2, 2)),
            pltpu.SemaphoreType.DMA((2,)),
            pltpu.SemaphoreType.DMA((2,)),
            pltpu.SemaphoreType.DMA((ITERS, 2)),
            pltpu.SemaphoreType.REGULAR,
        ],
        compiler_params=pltpu.CompilerParams(collective_id=0, has_side_effects=True),
        name="coupling",
    )(*vectors, args[5], args[6])

    def finish(a, b, c, d, sems):
        copies = [pltpu.make_async_copy(a, c, sems.at[0]), pltpu.make_async_copy(b, d, sems.at[1])]
        for copy in copies:
            copy.start()
        for copy in copies:
            copy.wait()

    outs = pl.pallas_call(
        finish,
        out_shape=[jax.ShapeDtypeStruct((groups, LANES), F32)] * 2,
        in_specs=[vmem_spec] * 2,
        out_specs=[any_spec] * 2,
        scratch_shapes=[pltpu.SemaphoreType.DMA((2,))],
        name="finish",
    )(*[pltpu.with_memory_space_constraint(o, pltpu.VMEM) for o in outs])
    return outs[0].reshape(width), outs[1].reshape(width)


def solution(mesh):
    one = P(AXES)
    return jax.shard_map(
        functools.partial(shards, mesh.shape["iface"], mesh.shape["dom"]),
        mesh=mesh,
        in_specs=(one,) * 5 + (P(None, AXES),) * 2,
        out_specs=(one, one),
        check_vma=False,
    )
```

```python
import functools
import jax
import jax.numpy as jnp
from jax import lax
from jax.experimental import pallas as pl
from jax.experimental.pallas import tpu as pltpu
from jax.sharding import PartitionSpec as P

ITERS = 3
coupling = 0.25
LANES = 128
AXES = ("iface", "dom")
F32 = jnp.float32
BF16 = jnp.bfloat16


def invert(matrix, rows):
    lane8 = lax.broadcasted_iota(jnp.int32, (8, LANES), 1)
    sub8 = lax.broadcasted_iota(jnp.int32, (8, LANES), 0)
    blocks = [matrix[8 * at : 8 * at + 8, :] for at in range(rows // 8)]
    for step in range(rows // 8):
        first = 8 * step
        inside = (lane8 >= first) & (lane8 < first + 8)
        unit = (lane8 - first == sub8).astype(F32)
        pivots = blocks[step]
        columns = [jnp.broadcast_to(pivots[:, first + at : first + at + 1], (8, LANES)) for at in range(8)]
        panel = jnp.where(inside, unit, pivots)
        for at in range(8):
            inverse = 1.0 / columns[at][at : at + 1, :]
            own = sub8 == at
            factor = columns[at]
            row = panel[at : at + 1, :] * inverse
            panel = jnp.where(own, row, panel - factor * row)
            for later in range(at + 1, 8):
                row = columns[later][at : at + 1, :] * inverse
                columns[later] = jnp.where(own, row, columns[later] - factor * row)
        for other in range(rows // 8):
            if other != step:
                block = blocks[other]
                total = jnp.where(inside, 0.0, block)
                for at in range(8):
                    column = jnp.broadcast_to(block[:, first + at : first + at + 1], (8, LANES))
                    total = total - column * panel[at : at + 1, :]
                blocks[other] = total
        blocks[step] = panel
    return jnp.concatenate(blocks, axis=0)


def kernel(
    sizes,
    interface,
    previous_residual,
    previous_estimate,
    forcing,
    stiffness,
    history_residual,
    history_estimate,
    next_ref,
    last_ref,
    cur,
    est,
    force,
    stiff,
    old_res,
    hist_v,
    hist_w,
    halo_w,
    new_v,
    new_w,
    edge_out,
    edge_in,
    dots_in,
    square,
    part_out,
    part_in,
    gathered,
    first_in,
    row_in,
    piece_sem,
    load_sem,
    edge_sem,
    wide_sem,
    part_sem,
    gather_sem,
    row_sem,
    go_sem,
):
    n_iface, n_dom, hist, base, rows, width, owners, share, depth = sizes
    count = n_iface * n_dom
    groups = width // LANES
    tall = groups + 8
    at_iface, at_dom = lax.axis_index("iface"), lax.axis_index("dom")
    me = at_iface * n_dom + at_dom
    last = count - 1
    n_own = len(owners)
    doms = [lax.rem(at_dom + step, n_dom) for step in range(n_dom)]
    low = at_iface < n_iface // 2
    others = []
    for step in range(n_iface - 1):
        down = n_iface - 1 - step
        others.append(
            jnp.where(low, jnp.where(down > at_iface, down, down - 1), jnp.where(step < at_iface, step, step + 1))
        )
    everyone = [(a, b) for a in others for b in doms] + [(at_iface, b) for b in doms[1:]]
    mine = [(at_iface == a) & (at_dom == b) for a, b in owners]
    owner = functools.reduce(jnp.logical_or, mine)
    slot = sum(jnp.where(yes, at, 0) for at, yes in enumerate(mine))

    def place(index):
        return (index // n_dom, lax.rem(index, n_dom))

    right = place(lax.rem(me + 1, count))
    left = place(lax.rem(me + last, count))

    def piece(at):
        span = pl.ds(at * depth, depth)
        return pltpu.make_async_copy(history_residual.at[:, span], hist_v.at[:, span], piece_sem.at[at])

    for at in range(width // depth):
        piece(at).start()
    inside = pl.ds(0, groups)
    small = []
    for at, (source, target) in enumerate(
        [
            (interface, cur.at[inside]),
            (previous_estimate, est.at[inside]),
            (forcing, force.at[inside]),
            (stiffness, stiff.at[inside]),
            (previous_residual, old_res),
        ]
    ):
        copy = pltpu.make_async_copy(source, target, load_sem.at[1 + at])
        copy.start()
        small.append(copy)
    load_w = pltpu.make_async_copy(history_estimate, hist_w, load_sem.at[0])

    barrier = pltpu.get_barrier_semaphore()

    def greet(device):
        pl.semaphore_signal(barrier, inc=1, device_id=device, device_id_type=pl.DeviceIdType.MESH)

    @pl.when(me < last)
    def _():
        greet(right)

    @pl.when(me > 0)
    def _():
        greet(left)

    @pl.when(owner)
    def _():
        for device in everyone:
            greet(device)

    @pl.when(jnp.logical_not(owner))
    def _():
        for device in owners:
            greet(device)

    main = side = None
    dims = (((1,), (1,)), ((), ()))
    for at in range(width // depth):
        piece(at).wait()
        block = hist_v[:, at * depth : (at + 1) * depth]
        one = block.astype(BF16)
        rest = block - one.astype(F32)
        two = rest.astype(BF16)
        three = (rest - two.astype(F32)).astype(BF16)
        for a, b, which in [(two, one, 1), (three, one, 1), (one, one, 0), (two, two, 0)]:
            term = lax.dot_general(a, b, dims, preferred_element_type=F32)
            if which == 0:
                main = term if main is None else main + term
            else:
                side = term if side is None else side + term
    load_w.start()
    square[...] = jnp.zeros(square.shape, F32)
    square[0:hist, 0:hist] = side
    mirrored = square[...].T
    square[0:hist, 0:hist] = main + side
    square[...] = square[...] + mirrored
    lane8 = lax.broadcasted_iota(jnp.int32, (8, LANES), 1)
    sub8 = lax.broadcasted_iota(jnp.int32, (8, LANES), 0)
    blocks = base // 8
    pairs = blocks // 2 + 1

    def lanes_of(block):
        return (lane8 >= 8 * block) & (lane8 < 8 * block + 8)

    for pair in range(n_own * share):
        packed = jnp.zeros((8, LANES), F32)
        for block in range(blocks if pair < pairs else 0):
            shown = lanes_of((block - pair) % blocks)
            packed = jnp.where(shown, square[8 * block : 8 * block + 8, :], packed)
        part_out[pair // share, pl.ds(8 * (pair % share), 8), :] = packed
    for copy in small:
        copy.wait()
    for at, ref in enumerate([cur, est, force, stiff]):
        edge_out[0, at : at + 1] = ref[groups - 1 : groups]
        edge_out[1, at : at + 1] = ref[0:1]
    pl.semaphore_wait(barrier, jnp.where(owner, last, n_own) + jnp.where(me < last, 1, 0) + jnp.where(me > 0, 1, 0))

    def remote(source, target, send_sem, recv_sem, device):
        return pltpu.make_async_remote_copy(
            src_ref=source,
            dst_ref=target,
            send_sem=send_sem,
            recv_sem=recv_sem,
            device_id=device,
            device_id_type=pl.DeviceIdType.MESH,
        )

    def send(source, target, sems, device):
        remote(source, target, sems.at[0], sems.at[1], device).start()

    def drain(target, many, sem):
        most = target.at[pl.ds(0, many)]
        pltpu.make_async_copy(most, most, sem).wait()

    def edges(sources, target, sems):
        return [
            remote(source, target.at[side], sems.at[0, side], sems.at[1, side], device)
            for side, (source, device) in enumerate(zip(sources, [right, left]))
        ]

    def edges_start(copies):
        for side, some in enumerate([me < last, me > 0]):

            @pl.when(some)
            def _():
                copies[side].start()

    def edges_wait(copies):
        for side, (sent, received) in enumerate([(me < last, me > 0), (me > 0, me < last)]):

            @pl.when(sent)
            def _():
                copies[side].wait_send()

            @pl.when(received)
            def _():
                copies[side].wait_recv()

    for at, yes in enumerate(mine):

        @pl.when(yes)
        def _():
            part_in[me] = part_out[at]

        @pl.when(jnp.logical_not(yes))
        def _():
            send(part_out.at[at], part_in.at[me], part_sem, owners[at])

    @pl.when(mine[0])
    def _():
        for device in everyone:
            pl.semaphore_signal(go_sem, inc=1, device_id=device, device_id_type=pl.DeviceIdType.MESH)

    halos = edges([edge_out.at[0], edge_out.at[1]], edge_in, edge_sem)
    edges_start(halos)
    tail = pl.ds(width - LANES, LANES)
    head = pl.ds(0, LANES)
    wide = edges([hist_w.at[:, tail], hist_w.at[:, head]], halo_w, wide_sem)

    half = LANES // 2
    from_right = lane8 < half
    valid = (from_right & (me < last)) | ((lane8 >= half) & (me > 0))
    row_at = lax.broadcasted_iota(jnp.int32, (rows, LANES), 0)
    lane_at = lax.broadcasted_iota(jnp.int32, (rows, LANES), 1)
    eye = (row_at == lane_at).astype(F32)

    def column_of(row):
        return jnp.broadcast_to(jnp.sum(eye * row, axis=1, keepdims=True), (rows, LANES))

    def over_rows(value):
        return jnp.sum(value, axis=0, keepdims=True)

    def as_block(row):
        return jnp.broadcast_to(row, (8, LANES))

    def project(refs):
        def add(at, totals):
            first = pl.multiple_of(8 * at, 8)
            chunks = [ref[pl.ds(first, 8), :] for ref in refs]
            totals = [list(some) for some in totals]
            columns = pl.ds(pl.multiple_of(8 * LANES * at, 8 * LANES), 8 * LANES)
            for group, first in enumerate(range(0, hist, 8)):
                block = hist_v[first : min(first + 8, hist), columns]
                for which, chunk in enumerate(chunks):
                    terms = [
                        block[:, inner * LANES : (inner + 1) * LANES] * chunk[inner : inner + 1, :]
                        for inner in range(8)
                    ]
                    while len(terms) > 1:
                        terms = [a + b for a, b in zip(terms[0::2], terms[1::2])]
                    totals[which][group] = totals[which][group] + terms[0]
            return totals

        zeros = [jnp.zeros((min(8, hist - first), LANES), F32) for first in range(0, hist, 8)]
        totals = lax.fori_loop(0, groups // 8, add, [list(zeros) for _ in refs])
        return [jnp.concatenate(some, axis=0) for some in totals]

    def lane_sums(value):
        return over_rows(jnp.concatenate([value, jnp.zeros((LANES - value.shape[0], LANES), F32)], axis=0).T)

    def begin(iteration):
        if iteration == 0:
            totals_before = project([old_res])[0]
        current = cur[...]
        sides = []
        for shift, edge_lane in [(1, 0), (-1, LANES - 1)]:
            rolled = pltpu.roll(current, shift % LANES, 1)
            moved = pltpu.roll(rolled, shift % tall, 0)
            lane = lax.broadcasted_iota(jnp.int32, (tall, LANES), 1)
            sides.append(jnp.where(lane == edge_lane, moved, rolled))
        estimate = force[...] + stiff[...] * jnp.tanh(current) + coupling * (sides[0] + sides[1])
        new_w[iteration] = estimate - est[...]
        est[...] = estimate
        residual = (estimate - current)[0:groups]
        fresh = residual - old_res[...]
        new_v[iteration] = fresh
        old_res[...] = residual
        extra = jnp.zeros((8, LANES), F32)
        for other in range(iteration + 1):
            row = fresh if other == iteration else new_v[other]
            for first, value in [(0, residual), (4, fresh)]:
                extra = jnp.where(sub8 == first + other, over_rows(row * value), extra)
        total = project([old_res])[0]
        sums = lane_sums(jnp.concatenate([total, jnp.zeros((base - hist, LANES), F32), extra], axis=0))
        dots_in[iteration, 0:1] = sums
        target = row_in.at[iteration - 1]
        source = dots_in.at[iteration, pl.ds(0, 1)]
        if iteration == 0:
            dots_in[0, 1:2] = lane_sums(totals_before)
            target, source = first_in, dots_in.at[0]

            @pl.when(jnp.logical_not(mine[0]))
            def _():
                pl.semaphore_wait(go_sem, 1)

            first_in[me] = dots_in[0]
        else:
            row_in[iteration - 1, me] = sums
        for device in everyone:
            send(source, target.at[me], row_sem.at[iteration], device)

    def sums_of(iteration):
        target = first_in if iteration == 0 else row_in.at[iteration - 1]
        drain(target, last, row_sem.at[iteration, 1])
        return jnp.sum(target[...], axis=0)

    edges_wait(halos)
    for at, ref in enumerate([cur, est, force, stiff]):
        both = jnp.where(from_right, edge_in[1, at : at + 1], edge_in[0, at : at + 1])
        ref[groups:tall] = jnp.where(valid, both, 0.0)
    begin(0)
    load_w.wait()
    edges_start(wide)

    @pl.when(owner)
    def _():
        drain(part_in, last, part_sem.at[1])
        gathered[slot] = jnp.sum(part_in[...], axis=0)
        for device in everyone:
            send(gathered.at[slot], gathered.at[slot], gather_sem, device)
        drain(gathered, n_own - 1, gather_sem.at[1])

    @pl.when(jnp.logical_not(owner))
    def _():
        drain(gathered, n_own, gather_sem.at[1])

    for block in range(blocks):
        row = jnp.zeros((8, LANES), F32)
        for pair in range(pairs):
            packed = gathered[pair // share, pl.ds(8 * (pair % share), 8), :]
            row = jnp.where(lanes_of((block - pair) % blocks), packed, row)
        square[8 * block : 8 * block + 8, :] = row
    square[base:LANES, :] = jnp.zeros((LANES - base, LANES), F32)
    shown = square[...]
    lane_block = lax.broadcasted_iota(jnp.int32, (LANES, LANES), 1) // 8
    row_block = lax.broadcasted_iota(jnp.int32, (LANES, LANES), 0) // 8
    ahead_by = row_block - lane_block
    ahead_by = jnp.where(ahead_by < 0, ahead_by + blocks, ahead_by)
    square[...] = jnp.where(ahead_by < pairs, shown, shown.T)
    kept = (row_at < hist) & (lane_at < hist)
    square[0:rows, :] = jnp.where(kept, square[0:rows, :], eye)
    square[0:base, :] = invert(square, base)
    square[0:rows, :] = jnp.where(kept, square[0:rows, :], 0.0)
    edges_wait(wide)
    halo_w[0] = jnp.where(
        lax.broadcasted_iota(jnp.int32, (hist, LANES), 1) < half, halo_w[1], halo_w[0]
    )

    def fold(parts):
        for step in (1, 2, 4):
            low = lax.rem(sub8, 2 * step) < step
            parts = [
                jnp.where(low, a, b) + pltpu.roll(jnp.where(low, b, a), step, 0)
                for a, b in zip(parts[0::2], parts[1::2])
            ]
        return parts[0]

    def solve(row):
        return jnp.broadcast_to(jnp.sum(square[0:base, :] * row, axis=1, keepdims=True), (base, LANES))

    solved, columns, lower, scale = [], [], [], []
    for iteration in range(ITERS):
        if iteration == 1:

            @pl.when(owner)
            def _():
                drain(gathered, n_own - 1, part_sem.at[0])
                drain(part_in, last, gather_sem.at[0])

            @pl.when(jnp.logical_not(owner))
            def _():
                drain(gathered, n_own, part_sem.at[0])

            drain(first_in, last, row_sem.at[0, 0])
        elif iteration > 1:
            drain(row_in.at[iteration - 2], last, row_sem.at[iteration - 1, 0])
        both = sums_of(iteration)
        proj = both[0:1, :]
        proj_sol = solve(proj)
        proj_col = column_of(proj)
        extra = proj_col[base:rows]
        proj_col = proj_col[0:base]
        if iteration == 0:
            before_sol, before_col = solve(both[1:2, :]), column_of(both[1:2, :])[0:base]
        solved.append(proj_sol - before_sol)
        columns.append(proj_col - before_col)
        before_sol, before_col = proj_sol, proj_col
        size = iteration + 1
        ahead = []
        for b in range(size):
            value = extra[4 + b : 5 + b, :] - over_rows(columns[b] * solved[iteration])
            for c in range(b if b < iteration else 0):
                value = value - ahead[c] * lower[b][c]
            ahead.append(value)
        lower.append([ahead[b] * scale[b] for b in range(iteration)])
        pivot = ahead[iteration]
        for b in range(iteration):
            pivot = pivot - ahead[b] * lower[iteration][b]
        scale.append(1.0 / pivot)
        answer = []
        for a in range(size):
            value = extra[a : a + 1, :] - over_rows(solved[a] * proj_col)
            for b in range(a):
                value = value - lower[a][b] * answer[b]
            answer.append(value)
        answer = [value * scale[a] for a, value in enumerate(answer)]
        for a in reversed(range(size)):
            for b in range(a + 1, size):
                answer[a] = answer[a] - lower[b][a] * answer[b]
        weights = proj_sol
        for a in range(size):
            weights = weights - solved[a] * answer[a]

        def weighted(ref, columns, many):
            totals = [None] * many
            for first in reversed(range(0, hist, 8)):
                some = min(8, hist - first)
                block = ref[first : first + some, columns]
                for inner in range(many):
                    term = block[:, inner * LANES : (inner + 1) * LANES] * weights[first : first + some, :]
                    if some < 8:
                        term = jnp.concatenate([term, jnp.zeros((8 - some, LANES), F32)], axis=0)
                    totals[inner] = term if totals[inner] is None else totals[inner] + term
            return totals

        def finished(where, total):
            for a in range(size):
                total = total + new_w[a, where, :] * answer[a]
            return est[where, :] - total

        def combine(at, carry):
            parts = weighted(hist_w, pl.ds(pl.multiple_of(8 * LANES * at, 8 * LANES), 8 * LANES), 8)
            where = pl.ds(pl.multiple_of(8 * at, 8), 8)
            cur[where, :] = finished(where, fold(parts))
            return carry

        lax.fori_loop(0, groups // 8, combine, 0)
        if iteration + 1 < ITERS:
            edge = as_block(over_rows(weighted(halo_w.at[0], slice(None), 1)[0]))
            cur[groups:tall] = jnp.where(valid, finished(pl.ds(groups, 8), edge), 0.0)
            begin(iteration + 1)
    next_ref[...] = cur[0:groups]
    last_ref[...] = old_res[...]

    drain(row_in.at[ITERS - 2], last, row_sem.at[ITERS - 1, 0])


def shards(n_iface, n_dom, *args):
    width = args[0].shape[0]
    hist = args[5].shape[0]
    base = -(-hist // 8) * 8
    rows = base + 8
    count = n_iface * n_dom
    pairs = base // 8 // 2 + 1
    middle = range(n_iface // 4, n_iface // 4 + max(1, n_iface // 2))
    owners = [(a, b) for a in middle for b in range(n_dom) if b % 2 == (n_dom > 1)][:pairs]
    share = -(-pairs // len(owners))
    depth = next(d for d in (2048, 1024) if width % d == 0)
    groups = width // LANES
    tall = groups + 8
    assert hist <= 112 and ITERS <= 4
    vectors = [a.reshape(groups, LANES) for a in args[:5]]
    any_spec = pl.BlockSpec(memory_space=pl.ANY)
    vmem_spec = pl.BlockSpec(memory_space=pltpu.VMEM)
    outs = pl.pallas_call(
        functools.partial(kernel, (n_iface, n_dom, hist, base, rows, width, owners, share, depth)),
        out_shape=[pltpu.VMEM((groups, LANES), F32)] * 2,
        in_specs=[any_spec] * 7,
        out_specs=[vmem_spec] * 2,
        scratch_shapes=[
            pltpu.VMEM((tall, LANES), F32),
            pltpu.VMEM((tall, LANES), F32),
            pltpu.VMEM((tall, LANES), F32),
            pltpu.VMEM((tall, LANES), F32),
            pltpu.VMEM((groups, LANES), F32),
            pltpu.VMEM((hist, width), F32),
            pltpu.VMEM((hist, width), F32),
            pltpu.VMEM((2, hist, LANES), F32),
            pltpu.VMEM((ITERS, groups, LANES), F32),
            pltpu.VMEM((ITERS, tall, LANES), F32),
            pltpu.VMEM((2, 8, LANES), F32),
            pltpu.VMEM((2, 8, LANES), F32),
            pltpu.VMEM((ITERS, 2, LANES), F32),
            pltpu.VMEM((LANES, LANES), F32),
            pltpu.VMEM((len(owners), 8 * share, LANES), F32),
            pltpu.VMEM((count, 8 * share, LANES), F32),
            pltpu.VMEM((len(owners), 8 * share, LANES), F32),
            pltpu.VMEM((count, 2, LANES), F32),
            pltpu.VMEM((ITERS - 1, count, 1, LANES), F32),
            pltpu.SemaphoreType.DMA((width // depth,)),
            pltpu.SemaphoreType.DMA((6,)),
            pltpu.SemaphoreType.DMA((2, 2)),
            pltpu.SemaphoreType.DMA((2, 2)),
            pltpu.SemaphoreType.DMA((2,)),
            pltpu.SemaphoreType.DMA((2,)),
            pltpu.SemaphoreType.DMA((ITERS, 2)),
            pltpu.SemaphoreType.REGULAR,
        ],
        compiler_params=pltpu.CompilerParams(collective_id=0, has_side_effects=True),
        name="coupling",
    )(*vectors, args[5], args[6])

    def finish(a, b, c, d, sems):
        copies = [pltpu.make_async_copy(a, c, sems.at[0]), pltpu.make_async_copy(b, d, sems.at[1])]
        for copy in copies:
            copy.start()
        for copy in copies:
            copy.wait()

    outs = pl.pallas_call(
        finish,
        out_shape=[jax.ShapeDtypeStruct((groups, LANES), F32)] * 2,
        in_specs=[vmem_spec] * 2,
        out_specs=[any_spec] * 2,
        scratch_shapes=[pltpu.SemaphoreType.DMA((2,))],
        name="finish",
    )(*[pltpu.with_memory_space_constraint(o, pltpu.VMEM) for o in outs])
    return outs[0].reshape(width), outs[1].reshape(width)


def solution(mesh):
    one = P(AXES)
    return jax.shard_map(
        functools.partial(shards, mesh.shape["iface"], mesh.shape["dom"]),
        mesh=mesh,
        in_specs=(one,) * 5 + (P(None, AXES),) * 2,
        out_specs=(one, one),
        check_vma=False,
    )
```

```python
import functools
import jax
import jax.numpy as jnp
from jax import lax
from jax.experimental import pallas as pl
from jax.experimental.pallas import tpu as pltpu
from jax.sharding import PartitionSpec as P

ITERS = 3
coupling = 0.25
LANES = 128
AXES = ("iface", "dom")
F32 = jnp.float32
BF16 = jnp.bfloat16


def invert(matrix, rows):
    lane8 = lax.broadcasted_iota(jnp.int32, (8, LANES), 1)
    sub8 = lax.broadcasted_iota(jnp.int32, (8, LANES), 0)
    many = rows // 8
    blocks = [matrix[8 * at : 8 * at + 8, :] for at in range(many)]
    def spread(block, lane):
        return jnp.broadcast_to(jnp.sum(jnp.where(lane8 == lane, block, 0.0), axis=1, keepdims=True), (8, LANES))
    columns = [spread(blocks[0], at) for at in range(8)]
    for step in range(many):
        first = 8 * step
        inside = (lane8 >= first) & (lane8 < first + 8)
        unit = (lane8 - first == sub8).astype(F32)
        panel = jnp.where(inside, unit, blocks[step])
        factors = [None if other == step else [spread(blocks[other], first + at) for at in range(8)] for other in range(many)]
        ahead = step + 1 < many
        if ahead:
            below = list(factors[step + 1])
            corner = [spread(blocks[step + 1], first + 8 + at) for at in range(8)]
        for at in range(8):
            inverse = 1.0 / columns[at][at : at + 1, :]
            own = sub8 == at
            factor = columns[at]
            row = panel[at : at + 1, :] * inverse
            panel = jnp.where(own, row, panel - factor * row)
            for later in range(at + 1, 8):
                row = columns[later][at : at + 1, :] * inverse
                columns[later] = jnp.where(own, row, columns[later] - factor * row)
                if ahead:
                    below[later] = below[later] - below[at] * row
            if ahead:
                scaled = below[at] * inverse
                for c in range(8):
                    corner[c] = corner[c] - below[at] * scaled[c : c + 1, :]
        for other in range(many):
            if other != step:
                total = jnp.where(inside, 0.0, blocks[other])
                terms = [factors[other][at] * panel[at : at + 1, :] for at in range(8)]
                if True:
                    while len(terms) > 1:
                        terms = [a + b for a, b in zip(terms[0::2], terms[1::2])]
                for term in terms:
                    total = total - term
                blocks[other] = total
        blocks[step] = panel
        if ahead:
            columns = corner
    return jnp.concatenate(blocks, axis=0)


def kernel(
    sizes,
    interface,
    previous_residual,
    previous_estimate,
    forcing,
    stiffness,
    history_residual,
    history_estimate,
    next_ref,
    last_ref,
    cur,
    est,
    force,
    stiff,
    old_res,
    hist_v,
    hist_w,
    halo_w,
    new_v,
    new_w,
    edge_out,
    edge_in,
    dots_in,
    square,
    part_out,
    part_in,
    gathered,
    first_in,
    row_in,
    piece_sem,
    load_sem,
    edge_sem,
    wide_sem,
    part_sem,
    gather_sem,
    row_sem,
    go_sem,
):
    n_iface, n_dom, hist, base, rows, width, owners, share, depths = sizes
    count = n_iface * n_dom
    groups = width // LANES
    tall = groups + 8
    at_iface, at_dom = lax.axis_index("iface"), lax.axis_index("dom")
    me = at_iface * n_dom + at_dom
    last = count - 1
    n_own = len(owners)
    doms = [lax.rem(at_dom + step, n_dom) for step in range(n_dom)]
    low = at_iface < n_iface // 2
    others = []
    for step in range(n_iface - 1):
        down = n_iface - 1 - step
        others.append(
            jnp.where(low, jnp.where(down > at_iface, down, down - 1), jnp.where(step < at_iface, step, step + 1))
        )
    everyone = [(a, b) for a in others for b in doms] + [(at_iface, b) for b in doms[1:]]
    mine = [(at_iface == a) & (at_dom == b) for a, b in owners]
    owner = functools.reduce(jnp.logical_or, mine)
    slot = sum(jnp.where(yes, at, 0) for at, yes in enumerate(mine))

    def place(index):
        return (index // n_dom, lax.rem(index, n_dom))

    right = place(lax.rem(me + 1, count))
    left = place(lax.rem(me + last, count))

    def piece(at):
        span = pl.ds(sum(depths[:at]), depths[at])
        return pltpu.make_async_copy(history_residual.at[:, span], hist_v.at[:, span], piece_sem.at[at])

    for at in range(len(depths)):
        piece(at).start()
    inside = pl.ds(0, groups)
    small = []
    for at, (source, target) in enumerate(
        [
            (interface, cur.at[inside]),
            (previous_estimate, est.at[inside]),
            (forcing, force.at[inside]),
            (stiffness, stiff.at[inside]),
            (previous_residual, old_res),
        ]
    ):
        copy = pltpu.make_async_copy(source, target, load_sem.at[1 + at])
        copy.start()
        small.append(copy)
    load_w = pltpu.make_async_copy(history_estimate, hist_w, load_sem.at[0])

    barrier = pltpu.get_barrier_semaphore()

    def greet(device):
        pl.semaphore_signal(barrier, inc=1, device_id=device, device_id_type=pl.DeviceIdType.MESH)

    @pl.when(me < last)
    def _():
        greet(right)

    @pl.when(me > 0)
    def _():
        greet(left)

    @pl.when(owner)
    def _():
        for device in everyone:
            greet(device)

    @pl.when(jnp.logical_not(owner))
    def _():
        for device in owners:
            greet(device)

    main = side = None
    dims = (((1,), (1,)), ((), ()))
    for at in range(len(depths)):
        piece(at).wait()
        block = hist_v[:, sum(depths[:at]) : sum(depths[: at + 1])]
        one = block.astype(BF16)
        rest = block - one.astype(F32)
        two = rest.astype(BF16)
        three = (rest - two.astype(F32)).astype(BF16)
        for a, b, which in [(two, one, 1), (three, one, 1), (one, one, 0), (two, two, 0)]:
            term = lax.dot_general(a, b, dims, preferred_element_type=F32)
            if which == 0:
                main = term if main is None else main + term
            else:
                side = term if side is None else side + term
    load_w.start()
    square[...] = jnp.zeros(square.shape, F32)
    square[0:hist, 0:hist] = side
    mirrored = square[...].T
    square[0:hist, 0:hist] = main + side
    square[...] = square[...] + mirrored
    lane8 = lax.broadcasted_iota(jnp.int32, (8, LANES), 1)
    sub8 = lax.broadcasted_iota(jnp.int32, (8, LANES), 0)
    blocks = base // 8
    pairs = blocks // 2 + 1

    def lanes_of(block):
        return (lane8 >= 8 * block) & (lane8 < 8 * block + 8)

    for pair in range(n_own * share):
        packed = jnp.zeros((8, LANES), F32)
        for block in range(blocks if pair < pairs else 0):
            shown = lanes_of((block - pair) % blocks)
            packed = jnp.where(shown, square[8 * block : 8 * block + 8, :], packed)
        part_out[pair // share, pl.ds(8 * (pair % share), 8), :] = packed
    for copy in small:
        copy.wait()
    for at, ref in enumerate([cur, est, force, stiff]):
        edge_out[0, at : at + 1] = ref[groups - 1 : groups]
        edge_out[1, at : at + 1] = ref[0:1]
    pl.semaphore_wait(barrier, jnp.where(owner, last, n_own) + jnp.where(me < last, 1, 0) + jnp.where(me > 0, 1, 0))

    def remote(source, target, send_sem, recv_sem, device):
        return pltpu.make_async_remote_copy(
            src_ref=source,
            dst_ref=target,
            send_sem=send_sem,
            recv_sem=recv_sem,
            device_id=device,
            device_id_type=pl.DeviceIdType.MESH,
        )

    def send(source, target, sems, device):
        remote(source, target, sems.at[0], sems.at[1], device).start()

    def drain(target, many, sem):
        most = target.at[pl.ds(0, many)]
        pltpu.make_async_copy(most, most, sem).wait()

    def edges(sources, target, sems):
        return [
            remote(source, target.at[side], sems.at[0, side], sems.at[1, side], device)
            for side, (source, device) in enumerate(zip(sources, [right, left]))
        ]

    def edges_start(copies):
        for side, some in enumerate([me < last, me > 0]):

            @pl.when(some)
            def _():
                copies[side].start()

    def edges_wait(copies):
        for side, (sent, received) in enumerate([(me < last, me > 0), (me > 0, me < last)]):

            @pl.when(sent)
            def _():
                copies[side].wait_send()

            @pl.when(received)
            def _():
                copies[side].wait_recv()

    for at, yes in enumerate(mine):

        @pl.when(yes)
        def _():
            part_in[me] = part_out[at]

        @pl.when(jnp.logical_not(yes))
        def _():
            send(part_out.at[at], part_in.at[me], part_sem, owners[at])

    @pl.when(mine[0])
    def _():
        for device in everyone:
            pl.semaphore_signal(go_sem, inc=1, device_id=device, device_id_type=pl.DeviceIdType.MESH)

    halos = edges([edge_out.at[0], edge_out.at[1]], edge_in, edge_sem)
    edges_start(halos)
    tail = pl.ds(width - LANES, LANES)
    head = pl.ds(0, LANES)
    wide = edges([hist_w.at[:, tail], hist_w.at[:, head]], halo_w, wide_sem)

    half = LANES // 2
    from_right = lane8 < half
    valid = (from_right & (me < last)) | ((lane8 >= half) & (me > 0))
    row_at = lax.broadcasted_iota(jnp.int32, (rows, LANES), 0)
    lane_at = lax.broadcasted_iota(jnp.int32, (rows, LANES), 1)
    eye = (row_at == lane_at).astype(F32)

    def column_of(row):
        return jnp.broadcast_to(jnp.sum(eye * row, axis=1, keepdims=True), (rows, LANES))

    def over_rows(value):
        return jnp.sum(value, axis=0, keepdims=True)

    def as_block(row):
        return jnp.broadcast_to(row, (8, LANES))

    def project(refs):
        def add(at, totals):
            first = 8 * at
            chunks = [ref[pl.ds(first, 8), :] for ref in refs]
            totals = [list(some) for some in totals]
            columns = pl.ds(8 * LANES * at, 8 * LANES)
            for group, first in enumerate(range(0, hist, 8)):
                block = hist_v[first : min(first + 8, hist), columns]
                for which, chunk in enumerate(chunks):
                    terms = [
                        block[:, inner * LANES : (inner + 1) * LANES] * chunk[inner : inner + 1, :]
                        for inner in range(8)
                    ]
                    while len(terms) > 1:
                        terms = [a + b for a, b in zip(terms[0::2], terms[1::2])]
                    totals[which][group] = totals[which][group] + terms[0]
            return totals

        zeros = [jnp.zeros((min(8, hist - first), LANES), F32) for first in range(0, hist, 8)]
        totals = [list(zeros) for _ in refs]
        for at in range(groups // 8):
            totals = add(at, totals)
        return [jnp.concatenate(some, axis=0) for some in totals]

    def lane_sums(value):
        return over_rows(jnp.concatenate([value, jnp.zeros((LANES - value.shape[0], LANES), F32)], axis=0).T)

    def begin(iteration):
        if iteration == 0:
            totals_before = project([old_res])[0]
        current = cur[...]
        sides = []
        for shift, edge_lane in [(1, 0), (-1, LANES - 1)]:
            rolled = pltpu.roll(current, shift % LANES, 1)
            moved = pltpu.roll(rolled, shift % tall, 0)
            lane = lax.broadcasted_iota(jnp.int32, (tall, LANES), 1)
            sides.append(jnp.where(lane == edge_lane, moved, rolled))
        estimate = force[...] + stiff[...] * jnp.tanh(current) + coupling * (sides[0] + sides[1])
        new_w[iteration] = estimate - est[...]
        est[...] = estimate
        residual = (estimate - current)[0:groups]
        fresh = residual - old_res[...]
        new_v[iteration] = fresh
        old_res[...] = residual
        extra = jnp.zeros((8, LANES), F32)
        for other in range(iteration + 1):
            row = fresh if other == iteration else new_v[other]
            for first, value in [(0, residual), (4, fresh)]:
                extra = jnp.where(sub8 == first + other, over_rows(row * value), extra)
        total = project([old_res])[0]
        sums = lane_sums(jnp.concatenate([total, jnp.zeros((base - hist, LANES), F32), extra], axis=0))
        dots_in[iteration, 0:1] = sums
        target = row_in.at[iteration - 1]
        source = dots_in.at[iteration, pl.ds(0, 1)]
        if iteration == 0:
            dots_in[0, 1:2] = lane_sums(totals_before)
            target, source = first_in, dots_in.at[0]

            @pl.when(jnp.logical_not(mine[0]))
            def _():
                pl.semaphore_wait(go_sem, 1)

            first_in[me] = dots_in[0]
        else:
            row_in[iteration - 1, me] = sums
        for device in everyone:
            send(source, target.at[me], row_sem.at[iteration], device)

    def sums_of(iteration):
        target = first_in if iteration == 0 else row_in.at[iteration - 1]
        drain(target, last, row_sem.at[iteration, 1])
        return jnp.sum(target[...], axis=0)

    edges_wait(halos)
    for at, ref in enumerate([cur, est, force, stiff]):
        both = jnp.where(from_right, edge_in[1, at : at + 1], edge_in[0, at : at + 1])
        ref[groups:tall] = jnp.where(valid, both, 0.0)
    begin(0)
    load_w.wait()
    edges_start(wide)
    @pl.when(owner)
    def _():
        drain(part_in, last, part_sem.at[1])
        gathered[slot] = jnp.sum(part_in[...], axis=0)
        for device in everyone:
            send(gathered.at[slot], gathered.at[slot], gather_sem, device)

    both = sums_of(0)
    row_first, row_before = both[0:1, :], both[1:2, :]
    col_first, col_before = column_of(row_first), column_of(row_before)[0:base]

    @pl.when(owner)
    def _():
        drain(gathered, n_own - 1, gather_sem.at[1])

    @pl.when(jnp.logical_not(owner))
    def _():
        drain(gathered, n_own, gather_sem.at[1])

    for block in range(blocks):
        row = jnp.zeros((8, LANES), F32)
        for pair in range(pairs):
            packed = gathered[pair // share, pl.ds(8 * (pair % share), 8), :]
            row = jnp.where(lanes_of((block - pair) % blocks), packed, row)
        square[8 * block : 8 * block + 8, :] = row
    square[base:LANES, :] = jnp.zeros((LANES - base, LANES), F32)
    shown = square[...]
    lane_block = lax.broadcasted_iota(jnp.int32, (LANES, LANES), 1) // 8
    row_block = lax.broadcasted_iota(jnp.int32, (LANES, LANES), 0) // 8
    ahead_by = row_block - lane_block
    ahead_by = jnp.where(ahead_by < 0, ahead_by + blocks, ahead_by)
    square[...] = jnp.where(ahead_by < pairs, shown, shown.T)
    kept = (row_at < hist) & (lane_at < hist)
    square[0:rows, :] = jnp.where(kept, square[0:rows, :], eye)
    square[0:base, :] = invert(square, base)
    square[0:rows, :] = jnp.where(kept, square[0:rows, :], 0.0)
    edges_wait(wide)
    halo_w[0] = jnp.where(
        lax.broadcasted_iota(jnp.int32, (hist, LANES), 1) < half, halo_w[1], halo_w[0]
    )

    def fold(parts):
        for step in (1, 2, 4):
            low = lax.rem(sub8, 2 * step) < step
            parts = [
                jnp.where(low, a, b) + pltpu.roll(jnp.where(low, b, a), step, 0)
                for a, b in zip(parts[0::2], parts[1::2])
            ]
        return parts[0]

    def solve(row):
        return jnp.broadcast_to(jnp.sum(square[0:base, :] * row, axis=1, keepdims=True), (base, LANES))

    solved, columns, lower, scale = [], [], [], []
    for iteration in range(ITERS):
        if iteration == 1:

            @pl.when(owner)
            def _():
                drain(gathered, n_own - 1, part_sem.at[0])
                drain(part_in, last, gather_sem.at[0])

            @pl.when(jnp.logical_not(owner))
            def _():
                drain(gathered, n_own, part_sem.at[0])

            drain(first_in, last, row_sem.at[0, 0])
        elif iteration > 1:
            drain(row_in.at[iteration - 2], last, row_sem.at[iteration - 1, 0])
        if iteration == 0:
            proj, proj_col, before_col = row_first, col_first, col_before
            before_sol = solve(row_before)
        else:
            proj = sums_of(iteration)
            proj_col = column_of(proj)
        proj_sol = solve(proj)
        extra = proj_col[base:rows]
        proj_col = proj_col[0:base]
        solved.append(proj_sol - before_sol)
        columns.append(proj_col - before_col)
        before_sol, before_col = proj_sol, proj_col
        size = iteration + 1
        ahead = []
        for b in range(size):
            value = extra[4 + b : 5 + b, :] - over_rows(columns[b] * solved[iteration])
            for c in range(b if b < iteration else 0):
                value = value - ahead[c] * lower[b][c]
            ahead.append(value)
        lower.append([ahead[b] * scale[b] for b in range(iteration)])
        pivot = ahead[iteration]
        for b in range(iteration):
            pivot = pivot - ahead[b] * lower[iteration][b]
        scale.append(1.0 / pivot)
        answer = []
        for a in range(size):
            value = extra[a : a + 1, :] - over_rows(solved[a] * proj_col)
            for b in range(a):
                value = value - lower[a][b] * answer[b]
            answer.append(value)
        answer = [value * scale[a] for a, value in enumerate(answer)]
        for a in reversed(range(size)):
            for b in range(a + 1, size):
                answer[a] = answer[a] - lower[b][a] * answer[b]
        weights = proj_sol
        for a in range(size):
            weights = weights - solved[a] * answer[a]

        def weighted(ref, columns, many):
            totals = [None] * many
            for first in reversed(range(0, hist, 8)):
                some = min(8, hist - first)
                block = ref[first : first + some, columns]
                for inner in range(many):
                    term = block[:, inner * LANES : (inner + 1) * LANES] * weights[first : first + some, :]
                    if some < 8:
                        term = jnp.concatenate([term, jnp.zeros((8 - some, LANES), F32)], axis=0)
                    totals[inner] = term if totals[inner] is None else totals[inner] + term
            return totals

        def finished(where, total):
            for a in range(size):
                total = total + new_w[a, where, :] * answer[a]
            return est[where, :] - total

        def combine(at, carry):
            parts = weighted(hist_w, pl.ds(8 * LANES * at, 8 * LANES), 8)
            where = pl.ds(8 * at, 8)
            cur[where, :] = finished(where, fold(parts))
            return carry

        for at in range(groups // 8):
            combine(at, 0)
        if iteration + 1 < ITERS:
            edge = as_block(over_rows(weighted(halo_w.at[0], slice(None), 1)[0]))
            cur[groups:tall] = jnp.where(valid, finished(pl.ds(groups, 8), edge), 0.0)
            begin(iteration + 1)
    next_ref[...] = cur[0:groups]
    last_ref[...] = old_res[...]

    drain(row_in.at[ITERS - 2], last, row_sem.at[ITERS - 1, 0])


def shards(n_iface, n_dom, *args):
    width = args[0].shape[0]
    hist = args[5].shape[0]
    base = -(-hist // 8) * 8
    rows = base + 8
    count = n_iface * n_dom
    pairs = base // 8 // 2 + 1
    middle = range(n_iface // 4, n_iface // 4 + max(1, n_iface // 2))
    owners = [(a, b) for a in middle for b in range(n_dom) if b % 2 == (n_dom > 1)][:pairs]
    share = -(-pairs // len(owners))
    assert width % (8 * LANES) == 0
    quarter = max(LANES, width // 4 // LANES * LANES)
    depths = [quarter, quarter, width - 2 * quarter]
    groups = width // LANES
    tall = groups + 8
    assert hist <= 112 and ITERS <= 4
    vectors = [a.reshape(groups, LANES) for a in args[:5]]
    any_spec = pl.BlockSpec(memory_space=pl.ANY)
    vmem_spec = pl.BlockSpec(memory_space=pltpu.VMEM)
    outs = pl.pallas_call(
        functools.partial(kernel, (n_iface, n_dom, hist, base, rows, width, owners, share, depths)),
        out_shape=[pltpu.VMEM((groups, LANES), F32)] * 2,
        in_specs=[any_spec] * 7,
        out_specs=[vmem_spec] * 2,
        scratch_shapes=[
            pltpu.VMEM((tall, LANES), F32),
            pltpu.VMEM((tall, LANES), F32),
            pltpu.VMEM((tall, LANES), F32),
            pltpu.VMEM((tall, LANES), F32),
            pltpu.VMEM((groups, LANES), F32),
            pltpu.VMEM((hist, width), F32),
            pltpu.VMEM((hist, width), F32),
            pltpu.VMEM((2, hist, LANES), F32),
            pltpu.VMEM((ITERS, groups, LANES), F32),
            pltpu.VMEM((ITERS, tall, LANES), F32),
            pltpu.VMEM((2, 8, LANES), F32),
            pltpu.VMEM((2, 8, LANES), F32),
            pltpu.VMEM((ITERS, 2, LANES), F32),
            pltpu.VMEM((LANES, LANES), F32),
            pltpu.VMEM((len(owners), 8 * share, LANES), F32),
            pltpu.VMEM((count, 8 * share, LANES), F32),
            pltpu.VMEM((len(owners), 8 * share, LANES), F32),
            pltpu.VMEM((count, 2, LANES), F32),
            pltpu.VMEM((ITERS - 1, count, 1, LANES), F32),
            pltpu.SemaphoreType.DMA((len(depths),)),
            pltpu.SemaphoreType.DMA((6,)),
            pltpu.SemaphoreType.DMA((2, 2)),
            pltpu.SemaphoreType.DMA((2, 2)),
            pltpu.SemaphoreType.DMA((2,)),
            pltpu.SemaphoreType.DMA((2,)),
            pltpu.SemaphoreType.DMA((ITERS, 2)),
            pltpu.SemaphoreType.REGULAR,
        ],
        compiler_params=pltpu.CompilerParams(collective_id=0, has_side_effects=True),
        name="coupling",
    )(*vectors, args[5], args[6])

    def finish(a, b, c, d, sems):
        copies = [pltpu.make_async_copy(a, c, sems.at[0]), pltpu.make_async_copy(b, d, sems.at[1])]
        for copy in copies:
            copy.start()
        for copy in copies:
            copy.wait()

    outs = pl.pallas_call(
        finish,
        out_shape=[jax.ShapeDtypeStruct((groups, LANES), F32)] * 2,
        in_specs=[vmem_spec] * 2,
        out_specs=[any_spec] * 2,
        scratch_shapes=[pltpu.SemaphoreType.DMA((2,))],
        name="finish",
    )(*[pltpu.with_memory_space_constraint(o, pltpu.VMEM) for o in outs])
    return outs[0].reshape(width), outs[1].reshape(width)


def solution(mesh):
    one = P(AXES)
    return jax.shard_map(
        functools.partial(shards, mesh.shape["iface"], mesh.shape["dom"]),
        mesh=mesh,
        in_specs=(one,) * 5 + (P(None, AXES),) * 2,
        out_specs=(one, one),
        check_vma=False,
    )
```

```python
import functools
import jax
import jax.numpy as jnp
from jax import lax
from jax.experimental import pallas as pl
from jax.experimental.pallas import tpu as pltpu
from jax.sharding import PartitionSpec as P

ITERS = 3
coupling = 0.25
LANES = 128
AXES = ("iface", "dom")
F32 = jnp.float32
BF16 = jnp.bfloat16


def invert(matrix, rows):
    lane8 = lax.broadcasted_iota(jnp.int32, (8, LANES), 1)
    sub8 = lax.broadcasted_iota(jnp.int32, (8, LANES), 0)
    many = rows // 8
    blocks = [matrix[8 * at : 8 * at + 8, :] for at in range(many)]
    def spread(block, lane):
        return jnp.broadcast_to(jnp.sum(jnp.where(lane8 == lane, block, 0.0), axis=1, keepdims=True), (8, LANES))
    columns = [spread(blocks[0], at) for at in range(8)]
    for step in range(many):
        first = 8 * step
        inside = (lane8 >= first) & (lane8 < first + 8)
        unit = (lane8 - first == sub8).astype(F32)
        panel = jnp.where(inside, unit, blocks[step])
        factors = [None if other == step else [spread(blocks[other], first + at) for at in range(8)] for other in range(many)]
        ahead = step + 1 < many
        if ahead:
            below = list(factors[step + 1])
            corner = [spread(blocks[step + 1], first + 8 + at) for at in range(8)]
        for at in range(8):
            inverse = 1.0 / columns[at][at : at + 1, :]
            own = sub8 == at
            factor = columns[at]
            row = panel[at : at + 1, :] * inverse
            panel = jnp.where(own, row, panel - factor * row)
            for later in range(at + 1, 8):
                row = columns[later][at : at + 1, :] * inverse
                columns[later] = jnp.where(own, row, columns[later] - factor * row)
                if ahead:
                    below[later] = below[later] - below[at] * row
            if ahead:
                scaled = below[at] * inverse
                for c in range(8):
                    corner[c] = corner[c] - below[at] * scaled[c : c + 1, :]
        for other in range(many):
            if other != step:
                total = jnp.where(inside, 0.0, blocks[other])
                terms = [factors[other][at] * panel[at : at + 1, :] for at in range(8)]
                if True:
                    while len(terms) > 1:
                        terms = [a + b for a, b in zip(terms[0::2], terms[1::2])]
                for term in terms:
                    total = total - term
                blocks[other] = total
        blocks[step] = panel
        if ahead:
            columns = corner
    return jnp.concatenate(blocks, axis=0)


def kernel(
    sizes,
    interface,
    previous_residual,
    previous_estimate,
    forcing,
    stiffness,
    history_residual,
    history_estimate,
    next_ref,
    last_ref,
    cur,
    est,
    force,
    stiff,
    old_res,
    hist_v,
    hist_w,
    halo_w,
    new_v,
    new_w,
    edge_out,
    edge_in,
    dots_in,
    square,
    part_out,
    part_in,
    gathered,
    first_in,
    row_in,
    piece_sem,
    load_sem,
    edge_sem,
    wide_sem,
    sent_sem,
    part_sem,
    gather_sem,
    row_sem,
    go_sem,
):
    n_iface, n_dom, hist, base, rows, width, owners, share, depths = sizes
    count = n_iface * n_dom
    groups = width // LANES
    tall = groups + 8
    at_iface, at_dom = lax.axis_index("iface"), lax.axis_index("dom")
    me = at_iface * n_dom + at_dom
    last = count - 1
    n_own = len(owners)
    doms = [lax.rem(at_dom + step, n_dom) for step in range(n_dom)]
    low = at_iface < n_iface // 2
    others = []
    for step in range(n_iface - 1):
        down = n_iface - 1 - step
        others.append(
            jnp.where(low, jnp.where(down > at_iface, down, down - 1), jnp.where(step < at_iface, step, step + 1))
        )
    everyone = [(a, b) for a in others for b in doms] + [(at_iface, b) for b in doms[1:]]
    mine = [(at_iface == a) & (at_dom == b) for a, b in owners]
    owner = functools.reduce(jnp.logical_or, mine)
    slot = sum(jnp.where(yes, at, 0) for at, yes in enumerate(mine))

    def place(index):
        return (index // n_dom, lax.rem(index, n_dom))

    right = place(lax.rem(me + 1, count))
    left = place(lax.rem(me + last, count))

    def piece(at):
        span = pl.ds(sum(depths[:at]), depths[at])
        return pltpu.make_async_copy(history_residual.at[:, span], hist_v.at[:, span], piece_sem.at[at])

    for at in range(len(depths)):
        piece(at).start()
    inside = pl.ds(0, groups)
    for source, target in (
        [
            (interface, cur.at[inside]),
            (previous_estimate, est.at[inside]),
            (forcing, force.at[inside]),
            (stiffness, stiff.at[inside]),
            (previous_residual, old_res),
        ]
    ):
        pltpu.make_async_copy(source, target, load_sem).start()
    load_w = pltpu.make_async_copy(history_estimate, hist_w, piece_sem.at[0])

    barrier = pltpu.get_barrier_semaphore()

    def greet(device):
        pl.semaphore_signal(barrier, inc=1, device_id=device, device_id_type=pl.DeviceIdType.MESH)

    @pl.when(me < last)
    def _():
        greet(right)

    @pl.when(me > 0)
    def _():
        greet(left)

    @pl.when(owner)
    def _():
        for device in everyone:
            greet(device)

    @pl.when(jnp.logical_not(owner))
    def _():
        for device in owners:
            greet(device)

    main = side = None
    dims = (((1,), (1,)), ((), ()))
    for at in range(len(depths)):
        piece(at).wait()
        block = hist_v[:, sum(depths[:at]) : sum(depths[: at + 1])]
        one = block.astype(BF16)
        rest = block - one.astype(F32)
        two = rest.astype(BF16)
        three = (rest - two.astype(F32)).astype(BF16)
        for a, b, which in [(two, one, 1), (three, one, 1), (one, one, 0), (two, two, 0)]:
            term = lax.dot_general(a, b, dims, preferred_element_type=F32)
            if which == 0:
                main = term if main is None else main + term
            else:
                side = term if side is None else side + term
    load_w.start()
    square[...] = jnp.zeros(square.shape, F32)
    square[0:hist, 0:hist] = side
    mirrored = square[...].T
    square[0:hist, 0:hist] = main + side
    square[...] = square[...] + mirrored
    lane8 = lax.broadcasted_iota(jnp.int32, (8, LANES), 1)
    sub8 = lax.broadcasted_iota(jnp.int32, (8, LANES), 0)
    blocks = base // 8
    pairs = blocks // 2 + 1

    def lanes_of(block):
        return (lane8 >= 8 * block) & (lane8 < 8 * block + 8)

    for pair in range(n_own * share):
        packed = jnp.zeros((8, LANES), F32)
        for block in range(blocks if pair < pairs else 0):
            shown = lanes_of((block - pair) % blocks)
            packed = jnp.where(shown, square[8 * block : 8 * block + 8, :], packed)
        part_out[pair // share, pl.ds(8 * (pair % share), 8), :] = packed
    together = hist_v.at[pl.ds(0, 8), pl.ds(0, 5 * width // 8)]
    pltpu.make_async_copy(together, together, load_sem).wait()
    for at, ref in enumerate([cur, est, force, stiff]):
        edge_out[0, at : at + 1] = ref[groups - 1 : groups]
        edge_out[1, at : at + 1] = ref[0:1]
    pl.semaphore_wait(barrier, jnp.where(owner, last, n_own) + jnp.where(me < last, 1, 0) + jnp.where(me > 0, 1, 0))

    def remote(source, target, send_sem, recv_sem, device):
        return pltpu.make_async_remote_copy(
            src_ref=source,
            dst_ref=target,
            send_sem=send_sem,
            recv_sem=recv_sem,
            device_id=device,
            device_id_type=pl.DeviceIdType.MESH,
        )

    def send(source, target, sem, device):
        remote(source, target, sent_sem, sem, device).start()

    def drain(target, many, sem):
        most = target.at[pl.ds(0, many)]
        pltpu.make_async_copy(most, most, sem).wait()

    def edges(sources, target, sem):
        return [
            remote(source, target.at[side], edge_sem.at[0, side], sem.at[side], device)
            for side, (source, device) in enumerate(zip(sources, [right, left]))
        ]

    def edges_start(copies):
        for side, some in enumerate([me < last, me > 0]):

            @pl.when(some)
            def _():
                copies[side].start()

    def edges_wait(copies):
        for side, (sent, received) in enumerate([(me < last, me > 0), (me > 0, me < last)]):

            @pl.when(sent)
            def _():
                copies[side].wait_send()

            @pl.when(received)
            def _():
                copies[side].wait_recv()

    for at, yes in enumerate(mine):

        @pl.when(yes)
        def _():
            part_in[me] = part_out[at]

        @pl.when(jnp.logical_not(yes))
        def _():
            send(part_out.at[at], part_in.at[me], part_sem, owners[at])

    @pl.when(mine[0])
    def _():
        for device in everyone:
            pl.semaphore_signal(go_sem, inc=1, device_id=device, device_id_type=pl.DeviceIdType.MESH)

    halos = edges([edge_out.at[0], edge_out.at[1]], edge_in, edge_sem.at[1])
    edges_start(halos)
    tail = pl.ds(width - LANES, LANES)
    head = pl.ds(0, LANES)
    wide = edges([hist_w.at[:, tail], hist_w.at[:, head]], halo_w, wide_sem)

    half = LANES // 2
    from_right = lane8 < half
    valid = (from_right & (me < last)) | ((lane8 >= half) & (me > 0))
    row_at = lax.broadcasted_iota(jnp.int32, (rows, LANES), 0)
    lane_at = lax.broadcasted_iota(jnp.int32, (rows, LANES), 1)
    eye = (row_at == lane_at).astype(F32)

    def column_of(row):
        return jnp.broadcast_to(jnp.sum(eye * row, axis=1, keepdims=True), (rows, LANES))

    def over_rows(value):
        return jnp.sum(value, axis=0, keepdims=True)

    def as_block(row):
        return jnp.broadcast_to(row, (8, LANES))

    def project(refs):
        def add(at, totals):
            first = 8 * at
            chunks = [ref[pl.ds(first, 8), :] for ref in refs]
            totals = [list(some) for some in totals]
            columns = pl.ds(8 * LANES * at, 8 * LANES)
            for group, first in enumerate(range(0, hist, 8)):
                block = hist_v[first : min(first + 8, hist), columns]
                for which, chunk in enumerate(chunks):
                    terms = [
                        block[:, inner * LANES : (inner + 1) * LANES] * chunk[inner : inner + 1, :]
                        for inner in range(8)
                    ]
                    while len(terms) > 1:
                        terms = [a + b for a, b in zip(terms[0::2], terms[1::2])]
                    totals[which][group] = totals[which][group] + terms[0]
            return totals

        zeros = [jnp.zeros((min(8, hist - first), LANES), F32) for first in range(0, hist, 8)]
        totals = [list(zeros) for _ in refs]
        for at in range(groups // 8):
            totals = add(at, totals)
        return [jnp.concatenate(some, axis=0) for some in totals]

    def lane_sums(value):
        return over_rows(jnp.concatenate([value, jnp.zeros((LANES - value.shape[0], LANES), F32)], axis=0).T)

    def begin(iteration):
        if iteration == 0:
            totals_before = project([old_res])[0]
        current = cur[...]
        sides = []
        for shift, edge_lane in [(1, 0), (-1, LANES - 1)]:
            rolled = pltpu.roll(current, shift % LANES, 1)
            moved = pltpu.roll(rolled, shift % tall, 0)
            lane = lax.broadcasted_iota(jnp.int32, (tall, LANES), 1)
            sides.append(jnp.where(lane == edge_lane, moved, rolled))
        estimate = force[...] + stiff[...] * jnp.tanh(current) + coupling * (sides[0] + sides[1])
        new_w[iteration] = estimate - est[...]
        est[...] = estimate
        residual = (estimate - current)[0:groups]
        fresh = residual - old_res[...]
        new_v[iteration] = fresh
        old_res[...] = residual
        extra = jnp.zeros((8, LANES), F32)
        for other in range(iteration + 1):
            row = fresh if other == iteration else new_v[other]
            for first, value in [(0, residual), (4, fresh)]:
                extra = jnp.where(sub8 == first + other, over_rows(row * value), extra)
        total = project([old_res])[0]
        sums = lane_sums(jnp.concatenate([total, jnp.zeros((base - hist, LANES), F32), extra], axis=0))
        dots_in[iteration, 0:1] = sums
        target = row_in.at[iteration - 1]
        source = dots_in.at[iteration, pl.ds(0, 1)]
        if iteration == 0:
            dots_in[0, 1:2] = lane_sums(totals_before)
            target, source = first_in, dots_in.at[0]

            @pl.when(jnp.logical_not(mine[0]))
            def _():
                pl.semaphore_wait(go_sem, 1)

            first_in[me] = dots_in[0]
        else:
            row_in[iteration - 1, me] = sums
        if iteration == 0:

            @pl.when(owner)
            def _():
                drain(gathered, n_own - 1, sent_sem)

            @pl.when(jnp.logical_not(owner))
            def _():
                drain(gathered, n_own, sent_sem)

        elif iteration == 1:

            @pl.when(owner)
            def _():
                drain(part_in, last, sent_sem)

        else:
            drain(row_in.at[iteration - 2], last, sent_sem)
        for device in everyone:
            send(source, target.at[me], row_sem.at[iteration % 2], device)

    def sums_of(iteration):
        target = first_in if iteration == 0 else row_in.at[iteration - 1]
        drain(target, last, row_sem.at[iteration % 2])
        return jnp.sum(target[...], axis=0)

    edges_wait(halos)
    for at, ref in enumerate([cur, est, force, stiff]):
        both = jnp.where(from_right, edge_in[1, at : at + 1], edge_in[0, at : at + 1])
        ref[groups:tall] = jnp.where(valid, both, 0.0)
    begin(0)
    load_w.wait()
    edges_start(wide)
    drain(first_in, last, sent_sem)
    @pl.when(owner)
    def _():
        drain(part_in, last, part_sem)
        gathered[slot] = jnp.sum(part_in[...], axis=0)
        for device in everyone:
            send(gathered.at[slot], gathered.at[slot], gather_sem, device)

    both = sums_of(0)
    row_first, row_before = both[0:1, :], both[1:2, :]
    col_first, col_before = column_of(row_first), column_of(row_before)[0:base]

    @pl.when(owner)
    def _():
        drain(gathered, n_own - 1, gather_sem)

    @pl.when(jnp.logical_not(owner))
    def _():
        drain(gathered, n_own, gather_sem)

    for block in range(blocks):
        row = jnp.zeros((8, LANES), F32)
        for pair in range(pairs):
            packed = gathered[pair // share, pl.ds(8 * (pair % share), 8), :]
            row = jnp.where(lanes_of((block - pair) % blocks), packed, row)
        square[8 * block : 8 * block + 8, :] = row
    square[base:LANES, :] = jnp.zeros((LANES - base, LANES), F32)
    shown = square[...]
    lane_block = lax.broadcasted_iota(jnp.int32, (LANES, LANES), 1) // 8
    row_block = lax.broadcasted_iota(jnp.int32, (LANES, LANES), 0) // 8
    ahead_by = row_block - lane_block
    ahead_by = jnp.where(ahead_by < 0, ahead_by + blocks, ahead_by)
    square[...] = jnp.where(ahead_by < pairs, shown, shown.T)
    kept = (row_at < hist) & (lane_at < hist)
    square[0:rows, :] = jnp.where(kept, square[0:rows, :], eye)
    square[0:base, :] = invert(square, base)
    square[0:rows, :] = jnp.where(kept, square[0:rows, :], 0.0)
    edges_wait(wide)
    halo_w[0] = jnp.where(
        lax.broadcasted_iota(jnp.int32, (hist, LANES), 1) < half, halo_w[1], halo_w[0]
    )

    def fold(parts):
        for step in (1, 2, 4):
            low = lax.rem(sub8, 2 * step) < step
            parts = [
                jnp.where(low, a, b) + pltpu.roll(jnp.where(low, b, a), step, 0)
                for a, b in zip(parts[0::2], parts[1::2])
            ]
        return parts[0]

    def solve(row):
        return jnp.broadcast_to(jnp.sum(square[0:base, :] * row, axis=1, keepdims=True), (base, LANES))

    solved, columns, lower, scale = [], [], [], []
    for iteration in range(ITERS):
        if iteration == 0:
            proj, proj_col, before_col = row_first, col_first, col_before
            before_sol = solve(row_before)
        else:
            proj = sums_of(iteration)
            proj_col = column_of(proj)
        proj_sol = solve(proj)
        extra = proj_col[base:rows]
        proj_col = proj_col[0:base]
        solved.append(proj_sol - before_sol)
        columns.append(proj_col - before_col)
        before_sol, before_col = proj_sol, proj_col
        size = iteration + 1
        ahead = []
        for b in range(size):
            value = extra[4 + b : 5 + b, :] - over_rows(columns[b] * solved[iteration])
            for c in range(b if b < iteration else 0):
                value = value - ahead[c] * lower[b][c]
            ahead.append(value)
        lower.append([ahead[b] * scale[b] for b in range(iteration)])
        pivot = ahead[iteration]
        for b in range(iteration):
            pivot = pivot - ahead[b] * lower[iteration][b]
        scale.append(1.0 / pivot)
        answer = []
        for a in range(size):
            value = extra[a : a + 1, :] - over_rows(solved[a] * proj_col)
            for b in range(a):
                value = value - lower[a][b] * answer[b]
            answer.append(value)
        answer = [value * scale[a] for a, value in enumerate(answer)]
        for a in reversed(range(size)):
            for b in range(a + 1, size):
                answer[a] = answer[a] - lower[b][a] * answer[b]
        weights = proj_sol
        for a in range(size):
            weights = weights - solved[a] * answer[a]

        def weighted(ref, columns, many):
            totals = [None] * many
            for first in reversed(range(0, hist, 8)):
                some = min(8, hist - first)
                block = ref[first : first + some, columns]
                for inner in range(many):
                    term = block[:, inner * LANES : (inner + 1) * LANES] * weights[first : first + some, :]
                    if some < 8:
                        term = jnp.concatenate([term, jnp.zeros((8 - some, LANES), F32)], axis=0)
                    totals[inner] = term if totals[inner] is None else totals[inner] + term
            return totals

        def finished(where, total):
            for a in range(size):
                total = total + new_w[a, where, :] * answer[a]
            return est[where, :] - total

        def combine(at, carry):
            parts = weighted(hist_w, pl.ds(8 * LANES * at, 8 * LANES), 8)
            where = pl.ds(8 * at, 8)
            cur[where, :] = finished(where, fold(parts))
            return carry

        for at in range(groups // 8):
            combine(at, 0)
        if iteration + 1 < ITERS:
            edge = as_block(over_rows(weighted(halo_w.at[0], slice(None), 1)[0]))
            cur[groups:tall] = jnp.where(valid, finished(pl.ds(groups, 8), edge), 0.0)
            begin(iteration + 1)
    next_ref[...] = cur[0:groups]
    last_ref[...] = old_res[...]

    drain(row_in.at[ITERS - 2], last, sent_sem)


def shards(n_iface, n_dom, *args):
    width = args[0].shape[0]
    hist = args[5].shape[0]
    base = -(-hist // 8) * 8
    rows = base + 8
    count = n_iface * n_dom
    pairs = base // 8 // 2 + 1
    middle = range(n_iface // 4, n_iface // 4 + max(1, n_iface // 2))
    owners = [(a, b) for a in middle for b in range(n_dom) if b % 2 == (n_dom > 1)][:pairs]
    share = -(-pairs // len(owners))
    assert width % (8 * LANES) == 0
    quarter = max(LANES, width // 4 // LANES * LANES)
    depths = [quarter, quarter, width - 2 * quarter]
    groups = width // LANES
    tall = groups + 8
    assert hist <= 112 and ITERS <= 4
    vectors = [a.reshape(groups, LANES) for a in args[:5]]
    any_spec = pl.BlockSpec(memory_space=pl.ANY)
    vmem_spec = pl.BlockSpec(memory_space=pltpu.VMEM)
    outs = pl.pallas_call(
        functools.partial(kernel, (n_iface, n_dom, hist, base, rows, width, owners, share, depths)),
        out_shape=[pltpu.VMEM((groups, LANES), F32)] * 2,
        in_specs=[any_spec] * 7,
        out_specs=[vmem_spec] * 2,
        scratch_shapes=[
            pltpu.VMEM((tall, LANES), F32),
            pltpu.VMEM((tall, LANES), F32),
            pltpu.VMEM((tall, LANES), F32),
            pltpu.VMEM((tall, LANES), F32),
            pltpu.VMEM((groups, LANES), F32),
            pltpu.VMEM((hist, width), F32),
            pltpu.VMEM((hist, width), F32),
            pltpu.VMEM((2, hist, LANES), F32),
            pltpu.VMEM((ITERS, groups, LANES), F32),
            pltpu.VMEM((ITERS, tall, LANES), F32),
            pltpu.VMEM((2, 8, LANES), F32),
            pltpu.VMEM((2, 8, LANES), F32),
            pltpu.VMEM((ITERS, 2, LANES), F32),
            pltpu.VMEM((LANES, LANES), F32),
            pltpu.VMEM((len(owners), 8 * share, LANES), F32),
            pltpu.VMEM((count, 8 * share, LANES), F32),
            pltpu.VMEM((len(owners), 8 * share, LANES), F32),
            pltpu.VMEM((count, 2, LANES), F32),
            pltpu.VMEM((ITERS - 1, count, 1, LANES), F32),
            pltpu.SemaphoreType.DMA((len(depths),)),
            pltpu.SemaphoreType.DMA,
            pltpu.SemaphoreType.DMA((2, 2)),
            pltpu.SemaphoreType.DMA((2,)),
            pltpu.SemaphoreType.DMA,
            pltpu.SemaphoreType.DMA,
            pltpu.SemaphoreType.DMA,
            pltpu.SemaphoreType.DMA((2,)),
            pltpu.SemaphoreType.REGULAR,
        ],
        compiler_params=pltpu.CompilerParams(collective_id=0, has_side_effects=True),
        name="coupling",
    )(*vectors, args[5], args[6])

    def finish(a, b, c, d, sems):
        copies = [pltpu.make_async_copy(a, c, sems.at[0]), pltpu.make_async_copy(b, d, sems.at[1])]
        for copy in copies:
            copy.start()
        for copy in copies:
            copy.wait()

    outs = pl.pallas_call(
        finish,
        out_shape=[jax.ShapeDtypeStruct((groups, LANES), F32)] * 2,
        in_specs=[vmem_spec] * 2,
        out_specs=[any_spec] * 2,
        scratch_shapes=[pltpu.SemaphoreType.DMA((2,))],
        name="finish",
    )(*[pltpu.with_memory_space_constraint(o, pltpu.VMEM) for o in outs])
    return outs[0].reshape(width), outs[1].reshape(width)


def solution(mesh):
    one = P(AXES)
    return jax.shard_map(
        functools.partial(shards, mesh.shape["iface"], mesh.shape["dom"]),
        mesh=mesh,
        in_specs=(one,) * 5 + (P(None, AXES),) * 2,
        out_specs=(one, one),
        check_vma=False,
    )
```

```python
import functools
import jax
import jax.numpy as jnp
from jax import lax
from jax.experimental import pallas as pl
from jax.experimental.pallas import tpu as pltpu
from jax.sharding import PartitionSpec as P

ITERS = 3
coupling = 0.25
LANES = 128
AXES = ("iface", "dom")
F32 = jnp.float32
BF16 = jnp.bfloat16


def invert(matrix, rows):
    lane8 = lax.broadcasted_iota(jnp.int32, (8, LANES), 1)
    sub8 = lax.broadcasted_iota(jnp.int32, (8, LANES), 0)
    many = rows // 8
    blocks = [matrix[8 * at : 8 * at + 8, :] for at in range(many)]
    def spread(block, lane):
        return jnp.broadcast_to(jnp.sum(jnp.where(lane8 == lane, block, 0.0), axis=1, keepdims=True), (8, LANES))
    columns = [spread(blocks[0], at) for at in range(8)]
    for step in range(many):
        first = 8 * step
        inside = (lane8 >= first) & (lane8 < first + 8)
        unit = (lane8 - first == sub8).astype(F32)
        panel = jnp.where(inside, unit, blocks[step])
        factors = [None if other == step else [spread(blocks[other], first + at) for at in range(8)] for other in range(many)]
        ahead = step + 1 < many
        if ahead:
            below = list(factors[step + 1])
            corner = [spread(blocks[step + 1], first + 8 + at) for at in range(8)]
        for at in range(8):
            inverse = 1.0 / columns[at][at : at + 1, :]
            own = sub8 == at
            factor = columns[at]
            row = panel[at : at + 1, :] * inverse
            panel = jnp.where(own, row, panel - factor * row)
            for later in range(at + 1, 8):
                row = columns[later][at : at + 1, :] * inverse
                columns[later] = jnp.where(own, row, columns[later] - factor * row)
                if ahead:
                    below[later] = below[later] - below[at] * row
            if ahead:
                scaled = below[at] * inverse
                for c in range(8):
                    corner[c] = corner[c] - below[at] * scaled[c : c + 1, :]
        for other in range(many):
            if other != step:
                total = jnp.where(inside, 0.0, blocks[other])
                terms = [factors[other][at] * panel[at : at + 1, :] for at in range(8)]
                if True:
                    while len(terms) > 1:
                        terms = [a + b for a, b in zip(terms[0::2], terms[1::2])]
                for term in terms:
                    total = total - term
                blocks[other] = total
        blocks[step] = panel
        if ahead:
            columns = corner
    return jnp.concatenate(blocks, axis=0)


def kernel(
    sizes,
    interface,
    previous_residual,
    previous_estimate,
    forcing,
    stiffness,
    history_residual,
    history_estimate,
    next_ref,
    last_ref,
    cur,
    est,
    force,
    stiff,
    old_res,
    hist_v,
    hist_w,
    halo_w,
    new_v,
    new_w,
    edge_out,
    edge_in,
    dots_in,
    square,
    part_out,
    part_in,
    gathered,
    first_in,
    row_in,
    piece_sem,
    load_sem,
    edge_sem,
    wide_sem,
    sent_sem,
    part_sem,
    gather_sem,
    row_sem,
    go_sem,
):
    n_iface, n_dom, hist, base, rows, width, owners, share, depths = sizes
    count = n_iface * n_dom
    groups = width // LANES
    tall = groups + 8
    at_iface, at_dom = lax.axis_index("iface"), lax.axis_index("dom")
    me = at_iface * n_dom + at_dom
    last = count - 1
    n_own = len(owners)
    doms = [lax.rem(at_dom + step, n_dom) for step in range(n_dom)]
    low = at_iface < n_iface // 2
    others = []
    for step in range(n_iface - 1):
        down = n_iface - 1 - step
        others.append(
            jnp.where(low, jnp.where(down > at_iface, down, down - 1), jnp.where(step < at_iface, step, step + 1))
        )
    everyone = [(a, b) for a in others for b in doms] + [(at_iface, b) for b in doms[1:]]
    mine = [(at_iface == a) & (at_dom == b) for a, b in owners]
    owner = functools.reduce(jnp.logical_or, mine)
    slot = sum(jnp.where(yes, at, 0) for at, yes in enumerate(mine))

    def place(index):
        return (index // n_dom, lax.rem(index, n_dom))

    right = place(lax.rem(me + 1, count))
    left = place(lax.rem(me + last, count))

    def piece(at):
        span = pl.ds(sum(depths[:at]), depths[at])
        return pltpu.make_async_copy(history_residual.at[:, span], hist_v.at[:, span], piece_sem.at[at])

    for at in range(len(depths)):
        piece(at).start()
    inside = pl.ds(0, groups)
    for source, target in (
        [
            (interface, cur.at[inside]),
            (previous_estimate, est.at[inside]),
            (forcing, force.at[inside]),
            (stiffness, stiff.at[inside]),
            (previous_residual, old_res),
        ]
    ):
        pltpu.make_async_copy(source, target, load_sem).start()
    load_w = pltpu.make_async_copy(history_estimate, hist_w, piece_sem.at[0])

    barrier = pltpu.get_barrier_semaphore()

    def greet(device):
        pl.semaphore_signal(barrier, inc=1, device_id=device, device_id_type=pl.DeviceIdType.MESH)

    @pl.when(me < last)
    def _():
        greet(right)

    @pl.when(me > 0)
    def _():
        greet(left)

    @pl.when(owner)
    def _():
        for device in everyone:
            greet(device)

    @pl.when(jnp.logical_not(owner))
    def _():
        for device in owners:
            greet(device)

    main = side = None
    dims = (((1,), (1,)), ((), ()))
    for at in range(len(depths)):
        piece(at).wait()
        block = hist_v[:, sum(depths[:at]) : sum(depths[: at + 1])]
        one = block.astype(BF16)
        rest = block - one.astype(F32)
        two = rest.astype(BF16)
        three = (rest - two.astype(F32)).astype(BF16)
        for a, b, which in [(two, one, 1), (three, one, 1), (one, one, 0), (two, two, 0)]:
            term = lax.dot_general(a, b, dims, preferred_element_type=F32)
            if which == 0:
                main = term if main is None else main + term
            else:
                side = term if side is None else side + term
    load_w.start()
    square[...] = jnp.zeros(square.shape, F32)
    square[0:hist, 0:hist] = side
    mirrored = square[...].T
    square[0:hist, 0:hist] = main + side
    square[...] = square[...] + mirrored
    lane8 = lax.broadcasted_iota(jnp.int32, (8, LANES), 1)
    sub8 = lax.broadcasted_iota(jnp.int32, (8, LANES), 0)
    blocks = base // 8
    pairs = blocks // 2 + 1

    def lanes_of(block):
        return (lane8 >= 8 * block) & (lane8 < 8 * block + 8)

    for pair in range(n_own * share):
        packed = jnp.zeros((8, LANES), F32)
        for block in range(blocks if pair < pairs else 0):
            shown = lanes_of((block - pair) % blocks)
            packed = jnp.where(shown, square[8 * block : 8 * block + 8, :], packed)
        part_out[pair // share, pl.ds(8 * (pair % share), 8), :] = packed
    together = hist_v.at[pl.ds(0, 8), pl.ds(0, 5 * width // 8)]
    pltpu.make_async_copy(together, together, load_sem).wait()
    for at, ref in enumerate([cur, est, force, stiff]):
        edge_out[0, at : at + 1] = ref[groups - 1 : groups]
        edge_out[1, at : at + 1] = ref[0:1]
    pl.semaphore_wait(barrier, jnp.where(owner, last, n_own) + jnp.where(me < last, 1, 0) + jnp.where(me > 0, 1, 0))

    def remote(source, target, send_sem, recv_sem, device):
        return pltpu.make_async_remote_copy(
            src_ref=source,
            dst_ref=target,
            send_sem=send_sem,
            recv_sem=recv_sem,
            device_id=device,
            device_id_type=pl.DeviceIdType.MESH,
        )

    def send(source, target, sem, device):
        remote(source, target, sent_sem, sem, device).start()

    def drain(target, many, sem):
        most = target.at[pl.ds(0, many)]
        pltpu.make_async_copy(most, most, sem).wait()

    def edges(sources, target, sem):
        return [
            remote(source, target.at[side], edge_sem.at[0, side], sem.at[side], device)
            for side, (source, device) in enumerate(zip(sources, [right, left]))
        ]

    def edges_start(copies):
        for side, some in enumerate([me < last, me > 0]):

            @pl.when(some)
            def _():
                copies[side].start()

    def edges_wait(copies):
        for side, (sent, received) in enumerate([(me < last, me > 0), (me > 0, me < last)]):

            @pl.when(sent)
            def _():
                copies[side].wait_send()

            @pl.when(received)
            def _():
                copies[side].wait_recv()

    for at, yes in enumerate(mine):

        @pl.when(yes)
        def _():
            part_in[me] = part_out[at]

        @pl.when(jnp.logical_not(yes))
        def _():
            send(part_out.at[at], part_in.at[me], part_sem, owners[at])

    @pl.when(mine[0])
    def _():
        for device in everyone:
            pl.semaphore_signal(go_sem, inc=1, device_id=device, device_id_type=pl.DeviceIdType.MESH)

    halos = edges([edge_out.at[0], edge_out.at[1]], edge_in, edge_sem.at[1])
    edges_start(halos)
    tail = pl.ds(width - LANES, LANES)
    head = pl.ds(0, LANES)
    wide = edges([hist_w.at[:, tail], hist_w.at[:, head]], halo_w, wide_sem)

    half = LANES // 2
    from_right = lane8 < half
    valid = (from_right & (me < last)) | ((lane8 >= half) & (me > 0))
    row_at = lax.broadcasted_iota(jnp.int32, (rows, LANES), 0)
    lane_at = lax.broadcasted_iota(jnp.int32, (rows, LANES), 1)
    eye = (row_at == lane_at).astype(F32)

    def column_of(row):
        return jnp.broadcast_to(jnp.sum(eye * row, axis=1, keepdims=True), (rows, LANES))

    def over_rows(value):
        return jnp.sum(value, axis=0, keepdims=True)

    def as_block(row):
        return jnp.broadcast_to(row, (8, LANES))

    def project(refs):
        def add(at, totals):
            first = 8 * at
            chunks = [ref[pl.ds(first, 8), :] for ref in refs]
            totals = [list(some) for some in totals]
            columns = pl.ds(8 * LANES * at, 8 * LANES)
            for group, first in enumerate(range(0, hist, 8)):
                block = hist_v[first : min(first + 8, hist), columns]
                for which, chunk in enumerate(chunks):
                    terms = [
                        block[:, inner * LANES : (inner + 1) * LANES] * chunk[inner : inner + 1, :]
                        for inner in range(8)
                    ]
                    while len(terms) > 1:
                        terms = [a + b for a, b in zip(terms[0::2], terms[1::2])]
                    totals[which][group] = totals[which][group] + terms[0]
            return totals

        zeros = [jnp.zeros((min(8, hist - first), LANES), F32) for first in range(0, hist, 8)]
        totals = [list(zeros) for _ in refs]
        for at in range(groups // 8):
            totals = add(at, totals)
        return [jnp.concatenate(some, axis=0) for some in totals]

    def lane_sums(value):
        return over_rows(jnp.concatenate([value, jnp.zeros((LANES - value.shape[0], LANES), F32)], axis=0).T)

    def begin(iteration):
        if iteration == 0:
            totals_before = project([old_res])[0]
        current = cur[...]
        sides = []
        for shift, edge_lane in [(1, 0), (-1, LANES - 1)]:
            rolled = pltpu.roll(current, shift % LANES, 1)
            moved = pltpu.roll(rolled, shift % tall, 0)
            lane = lax.broadcasted_iota(jnp.int32, (tall, LANES), 1)
            sides.append(jnp.where(lane == edge_lane, moved, rolled))
        estimate = force[...] + stiff[...] * jnp.tanh(current) + coupling * (sides[0] + sides[1])
        new_w[iteration] = estimate - est[...]
        est[...] = estimate
        residual = (estimate - current)[0:groups]
        fresh = residual - old_res[...]
        new_v[iteration] = fresh
        old_res[...] = residual
        extra = jnp.zeros((8, LANES), F32)
        for other in range(iteration + 1):
            row = fresh if other == iteration else new_v[other]
            for first, value in [(0, residual), (4, fresh)]:
                extra = jnp.where(sub8 == first + other, over_rows(row * value), extra)
        total = project([old_res])[0]
        sums = lane_sums(jnp.concatenate([total, jnp.zeros((base - hist, LANES), F32), extra], axis=0))
        dots_in[iteration, 0:1] = sums
        target = row_in.at[iteration - 1]
        source = dots_in.at[iteration, pl.ds(0, 1)]
        if iteration == 0:
            dots_in[0, 1:2] = lane_sums(totals_before)
            target, source = first_in, dots_in.at[0]

            @pl.when(jnp.logical_not(mine[0]))
            def _():
                pl.semaphore_wait(go_sem, 1)

            first_in[me] = dots_in[0]
        else:
            row_in[iteration - 1, me] = sums
        if iteration == 0:

            @pl.when(owner)
            def _():
                drain(gathered, n_own - 1, sent_sem)

            @pl.when(jnp.logical_not(owner))
            def _():
                drain(gathered, n_own, sent_sem)

        elif iteration == 1:

            @pl.when(owner)
            def _():
                drain(part_in, last, sent_sem)

        else:
            drain(row_in.at[iteration - 2], last, sent_sem)
        for device in everyone:
            send(source, target.at[me], row_sem.at[iteration % 2], device)

    def sums_of(iteration):
        target = first_in if iteration == 0 else row_in.at[iteration - 1]
        drain(target, last, row_sem.at[iteration % 2])
        return jnp.sum(target[...], axis=0)

    edges_wait(halos)
    for at, ref in enumerate([cur, est, force, stiff]):
        both = jnp.where(from_right, edge_in[1, at : at + 1], edge_in[0, at : at + 1])
        ref[groups:tall] = jnp.where(valid, both, 0.0)
    begin(0)
    load_w.wait()
    edges_start(wide)
    drain(first_in, last, sent_sem)
    @pl.when(owner)
    def _():
        drain(part_in, last, part_sem)
        gathered[slot] = jnp.sum(part_in[...], axis=0)
        for device in everyone:
            send(gathered.at[slot], gathered.at[slot], gather_sem, device)

    both = sums_of(0)
    row_first, row_before = both[0:1, :], both[1:2, :]
    col_first, col_before = column_of(row_first), column_of(row_before)[0:base]

    @pl.when(owner)
    def _():
        drain(gathered, n_own - 1, gather_sem)

    @pl.when(jnp.logical_not(owner))
    def _():
        drain(gathered, n_own, gather_sem)

    for block in range(blocks):
        row = jnp.zeros((8, LANES), F32)
        for pair in range(pairs):
            packed = gathered[pair // share, pl.ds(8 * (pair % share), 8), :]
            row = jnp.where(lanes_of((block - pair) % blocks), packed, row)
        square[8 * block : 8 * block + 8, :] = row
    square[base:LANES, :] = jnp.zeros((LANES - base, LANES), F32)
    shown = square[...]
    lane_block = lax.broadcasted_iota(jnp.int32, (LANES, LANES), 1) // 8
    row_block = lax.broadcasted_iota(jnp.int32, (LANES, LANES), 0) // 8
    ahead_by = row_block - lane_block
    ahead_by = jnp.where(ahead_by < 0, ahead_by + blocks, ahead_by)
    square[...] = jnp.where(ahead_by < pairs, shown, shown.T)
    kept = (row_at < hist) & (lane_at < hist)
    square[0:rows, :] = jnp.where(kept, square[0:rows, :], eye)
    square[0:base, :] = invert(square, base)
    square[0:rows, :] = jnp.where(kept, square[0:rows, :], 0.0)
    edges_wait(wide)
    halo_w[0] = jnp.where(
        lax.broadcasted_iota(jnp.int32, (hist, LANES), 1) < half, halo_w[1], halo_w[0]
    )

    def fold(parts):
        for step in (1, 2, 4):
            low = lax.rem(sub8, 2 * step) < step
            parts = [
                jnp.where(low, a, b) + pltpu.roll(jnp.where(low, b, a), step, 0)
                for a, b in zip(parts[0::2], parts[1::2])
            ]
        return parts[0]

    def solve(row):
        return jnp.broadcast_to(jnp.sum(square[0:base, :] * row, axis=1, keepdims=True), (base, LANES))

    solved, columns, lower, scale = [], [], [], []
    for iteration in range(ITERS):
        if iteration == 0:
            proj, proj_col, before_col = row_first, col_first, col_before
            before_sol = solve(row_before)
        else:
            proj = sums_of(iteration)
            proj_col = column_of(proj)
        proj_sol = solve(proj)
        extra = proj_col[base:rows]
        proj_col = proj_col[0:base]
        solved.append(proj_sol - before_sol)
        columns.append(proj_col - before_col)
        before_sol, before_col = proj_sol, proj_col
        size = iteration + 1
        ahead = []
        for b in range(size):
            value = extra[4 + b : 5 + b, :] - over_rows(columns[b] * solved[iteration])
            for c in range(b if b < iteration else 0):
                value = value - ahead[c] * lower[b][c]
            ahead.append(value)
        lower.append([ahead[b] * scale[b] for b in range(iteration)])
        pivot = ahead[iteration]
        for b in range(iteration):
            pivot = pivot - ahead[b] * lower[iteration][b]
        scale.append(1.0 / pivot)
        answer = []
        for a in range(size):
            value = extra[a : a + 1, :] - over_rows(solved[a] * proj_col)
            for b in range(a):
                value = value - lower[a][b] * answer[b]
            answer.append(value)
        answer = [value * scale[a] for a, value in enumerate(answer)]
        for a in reversed(range(size)):
            for b in range(a + 1, size):
                answer[a] = answer[a] - lower[b][a] * answer[b]
        weights = proj_sol
        for a in range(size):
            weights = weights - solved[a] * answer[a]

        def weighted(ref, columns, many):
            totals = [None] * many
            for first in reversed(range(0, hist, 8)):
                some = min(8, hist - first)
                block = ref[first : first + some, columns]
                for inner in range(many):
                    term = block[:, inner * LANES : (inner + 1) * LANES] * weights[first : first + some, :]
                    if some < 8:
                        term = jnp.concatenate([term, jnp.zeros((8 - some, LANES), F32)], axis=0)
                    totals[inner] = term if totals[inner] is None else totals[inner] + term
            return totals

        def finished(where, total):
            for a in range(size):
                total = total + new_w[a, where, :] * answer[a]
            return est[where, :] - total

        def combine(at, carry):
            parts = weighted(hist_w, pl.ds(8 * LANES * at, 8 * LANES), 8)
            where = pl.ds(8 * at, 8)
            cur[where, :] = finished(where, fold(parts))
            return carry

        for at in range(groups // 8):
            combine(at, 0)
        if iteration + 1 < ITERS:
            edge = as_block(over_rows(weighted(halo_w.at[0], slice(None), 1)[0]))
            cur[groups:tall] = jnp.where(valid, finished(pl.ds(groups, 8), edge), 0.0)
            begin(iteration + 1)
    next_ref[...] = cur[0:groups]
    last_ref[...] = old_res[...]

    drain(row_in.at[ITERS - 2], last, sent_sem)


def shards(n_iface, n_dom, *args):
    width = args[0].shape[0]
    hist = args[5].shape[0]
    base = -(-hist // 8) * 8
    rows = base + 8
    count = n_iface * n_dom
    pairs = base // 8 // 2 + 1
    middle = range(n_iface // 4, n_iface // 4 + max(1, n_iface // 2))
    owners = [(a, b) for a in reversed(middle) for b in range(n_dom) if b % 2 == (n_dom > 1)][:pairs]
    share = -(-pairs // len(owners))
    assert width % (8 * LANES) == 0
    quarter = max(LANES, width // 4 // LANES * LANES)
    depths = [quarter, quarter, width - 2 * quarter]
    groups = width // LANES
    tall = groups + 8
    assert hist <= 112 and ITERS <= 4
    vectors = [a.reshape(groups, LANES) for a in args[:5]]
    any_spec = pl.BlockSpec(memory_space=pl.ANY)
    vmem_spec = pl.BlockSpec(memory_space=pltpu.VMEM)
    outs = pl.pallas_call(
        functools.partial(kernel, (n_iface, n_dom, hist, base, rows, width, owners, share, depths)),
        out_shape=[pltpu.VMEM((groups, LANES), F32)] * 2,
        in_specs=[any_spec] * 7,
        out_specs=[vmem_spec] * 2,
        scratch_shapes=[
            pltpu.VMEM((tall, LANES), F32),
            pltpu.VMEM((tall, LANES), F32),
            pltpu.VMEM((tall, LANES), F32),
            pltpu.VMEM((tall, LANES), F32),
            pltpu.VMEM((groups, LANES), F32),
            pltpu.VMEM((hist, width), F32),
            pltpu.VMEM((hist, width), F32),
            pltpu.VMEM((2, hist, LANES), F32),
            pltpu.VMEM((ITERS, groups, LANES), F32),
            pltpu.VMEM((ITERS, tall, LANES), F32),
            pltpu.VMEM((2, 8, LANES), F32),
            pltpu.VMEM((2, 8, LANES), F32),
            pltpu.VMEM((ITERS, 2, LANES), F32),
            pltpu.VMEM((LANES, LANES), F32),
            pltpu.VMEM((len(owners), 8 * share, LANES), F32),
            pltpu.VMEM((count, 8 * share, LANES), F32),
            pltpu.VMEM((len(owners), 8 * share, LANES), F32),
            pltpu.VMEM((count, 2, LANES), F32),
            pltpu.VMEM((ITERS - 1, count, 1, LANES), F32),
            pltpu.SemaphoreType.DMA((len(depths),)),
            pltpu.SemaphoreType.DMA,
            pltpu.SemaphoreType.DMA((2, 2)),
            pltpu.SemaphoreType.DMA((2,)),
            pltpu.SemaphoreType.DMA,
            pltpu.SemaphoreType.DMA,
            pltpu.SemaphoreType.DMA,
            pltpu.SemaphoreType.DMA((2,)),
            pltpu.SemaphoreType.REGULAR,
        ],
        compiler_params=pltpu.CompilerParams(collective_id=0, has_side_effects=True),
        name="coupling",
    )(*vectors, args[5], args[6])

    def finish(a, b, c, d, sems):
        copies = [pltpu.make_async_copy(a, c, sems.at[0]), pltpu.make_async_copy(b, d, sems.at[1])]
        for copy in copies:
            copy.start()
        for copy in copies:
            copy.wait()

    outs = pl.pallas_call(
        finish,
        out_shape=[jax.ShapeDtypeStruct((groups, LANES), F32)] * 2,
        in_specs=[vmem_spec] * 2,
        out_specs=[any_spec] * 2,
        scratch_shapes=[pltpu.SemaphoreType.DMA((2,))],
        name="finish",
    )(*[pltpu.with_memory_space_constraint(o, pltpu.VMEM) for o in outs])
    return outs[0].reshape(width), outs[1].reshape(width)


def solution(mesh):
    one = P(AXES)
    return jax.shard_map(
        functools.partial(shards, mesh.shape["iface"], mesh.shape["dom"]),
        mesh=mesh,
        in_specs=(one,) * 5 + (P(None, AXES),) * 2,
        out_specs=(one, one),
        check_vma=False,
    )
```
